64 devices in a mesh: dp: 4 (over x, y), ep: 16 (over z, core).
Axes of the slice: x: 2, y: 2, z: 8, core: 2. Of those that a mesh axis runs over, the one named last changes fastest.
The devices are a block of a 4x4x8 slice.
Arguments:
- tokens: bfloat16 [16384, 2048], P(('dp', 'ep')), parts along dimension 0
- expert_ids: int32 [16384, 8], P(('dp', 'ep')), parts along dimension 0
- gate_wts: float32 [16384, 8], P(('dp', 'ep')), parts along dimension 0
- slot_ids: int32 [16384, 8], P(('dp', 'ep')), parts along dimension 0
- w_gate: bfloat16 [64, 2048, 1024], P('ep')
- w_up: bfloat16 [64, 2048, 1024], P('ep')
- w_down: bfloat16 [64, 1024, 2048], P('ep')
Outputs:
- output: bfloat16 [16384, 2048], P(('dp', 'ep')), parts along dimension 0
There are 4 independent parts. The reference program is written for one: setup_inputs(seed, part) draws one part's arguments, and reference() takes and returns one part's arrays. A program takes and returns all parts, laid end to end along the dimension named above; an argument that names none is the same for every part.
All inputs are finite; a program needn't handle non-finite values.
Results may differ from the reference program's by a relative error of at most 0.001.
Values are sent between devices in bfloat16 or wider.
A program may use at most 768 MiB of HBM per device.

```python
import jax
import jax.numpy as jnp
from jax import lax

GROUP_SIZE = 16
TOK_DEV = 256
D_MODEL = 2048
FF_DIM = 1024
EXPERTS = 64
TOP_K = 8

TOKENS = GROUP_SIZE * TOK_DEV
SHARD_CAP = 3 * TOK_DEV * TOP_K // (2 * EXPERTS)
CAPACITY = GROUP_SIZE * SHARD_CAP


def draw_routing(route_key, relabel_key):
    relabel = jax.random.permutation(relabel_key, EXPERTS)
    half_a = TOK_DEV // (2 * EXPERTS)
    hot_rows = 3 * half_a
    split_at = hot_rows * (EXPERTS // 2)
    tok_ids = jnp.arange(TOK_DEV)
    base_ids = jnp.where(tok_ids < split_at, tok_ids // hot_rows, EXPERTS // 2 + (tok_ids - split_at) // half_a)
    choice_off = jnp.arange(TOP_K)
    expert_axis = jnp.arange(EXPERTS)

    def one_shard(shard_num):
        shard_key = jax.random.fold_in(route_key, shard_num)
        perm_key, drop_key = jax.random.split(shard_key)
        tok_order = jax.random.permutation(perm_key, TOK_DEV)
        raw_ids = (base_ids[tok_order][:, None] + choice_off[None, :]) % EXPERTS
        drop_draw = jax.random.randint(drop_key, (TOK_DEV, TOP_K), 0, 8)
        keep_mask = (drop_draw != 0) | (raw_ids == TOP_K - 1)
        onehot = ((raw_ids.reshape(-1)[:, None] == expert_axis[None, :]) & keep_mask.reshape(-1)[:, None]).astype(jnp.int32)
        slot_rank = jnp.sum((jnp.cumsum(onehot, axis=0) - onehot) * onehot, axis=1).reshape(TOK_DEV, TOP_K)
        slot_ids = jnp.where(keep_mask, shard_num * SHARD_CAP + slot_rank, -1)
        return relabel[raw_ids].astype(jnp.int32), slot_ids.astype(jnp.int32)

    expert_ids, slot_ids = lax.map(one_shard, jnp.arange(GROUP_SIZE))
    return expert_ids.reshape(TOKENS, TOP_K), slot_ids.reshape(TOKENS, TOP_K)


def draw_weights(weight_key, shape_in, shape_out):
    def one_expert(expert_num):
        draw = jax.random.normal(jax.random.fold_in(weight_key, expert_num), (shape_in, shape_out), jnp.float32)
        return (draw * shape_in ** -0.5).astype(jnp.bfloat16)
    return lax.map(one_expert, jnp.arange(EXPERTS))


def setup_inputs(seed: int = 0, part: int = 0) -> dict:
    root_key = jax.random.key(seed)
    part_keys = jax.random.split(jax.random.fold_in(root_key, part), 4)
    weight_keys = jax.random.split(jax.random.key(seed + 1), 3)
    tokens = jax.random.normal(part_keys[0], (TOKENS, D_MODEL), jnp.float32).astype(jnp.bfloat16)
    gate_wts = jax.random.uniform(part_keys[1], (TOKENS, TOP_K), jnp.float32, minval=0.25, maxval=1.0) * TOP_K ** -0.5
    expert_ids, slot_ids = draw_routing(part_keys[2], part_keys[3])
    return {'tokens': tokens, 'expert_ids': expert_ids, 'gate_wts': gate_wts, 'slot_ids': slot_ids, 'w_gate': draw_weights(weight_keys[0], D_MODEL, FF_DIM), 'w_up': draw_weights(weight_keys[1], D_MODEL, FF_DIM), 'w_down': draw_weights(weight_keys[2], FF_DIM, D_MODEL)}


def reference(tokens, expert_ids, gate_wts, slot_ids, w_gate, w_up, w_down):
    keep_mask = slot_ids >= 0
    flat_slot = jnp.where(keep_mask, expert_ids * CAPACITY + slot_ids, EXPERTS * CAPACITY).reshape(-1)
    tok_index = jnp.broadcast_to(jnp.arange(TOKENS, dtype=jnp.int32)[:, None], expert_ids.shape).reshape(-1)
    slot_token = jnp.full((EXPERTS * CAPACITY,), TOKENS, jnp.int32).at[flat_slot].set(tok_index, mode='drop')
    slot_gate = jnp.zeros((EXPERTS * CAPACITY,), jnp.float32).at[flat_slot].set(gate_wts.reshape(-1), mode='drop')

    def expert_step(accum, scan_in):
        tok_rows, gate_rows, wg_one, wu_one, wd_one = scan_in
        buffer = jnp.take(tokens, tok_rows, axis=0, mode='fill', fill_value=0)
        h_gate = jnp.dot(buffer, wg_one, preferred_element_type=jnp.float32)
        h_up = jnp.dot(buffer, wu_one, preferred_element_type=jnp.float32)
        hidden = (jax.nn.silu(h_gate) * h_up).astype(jnp.bfloat16)
        expert_out = jnp.dot(hidden, wd_one, preferred_element_type=jnp.float32)
        accum = accum.at[tok_rows].add(expert_out * gate_rows[:, None], mode='drop')
        return accum, None

    accum, _ = lax.scan(expert_step, jnp.zeros((TOKENS, D_MODEL), jnp.float32), (slot_token.reshape(EXPERTS, CAPACITY), slot_gate.reshape(EXPERTS, CAPACITY), w_gate, w_up, w_down))
    return accum.astype(jnp.bfloat16)
```

```python
import functools

import jax
import jax.numpy as jnp
from jax import lax
from jax.experimental import pallas as pl
from jax.experimental.pallas import tpu as pltpu
from jax.sharding import PartitionSpec as P

CAP_NUM = 3
CAP_DEN = 2
COLS = 256
AG_CHUNKS = 2
SIB_SLOTS = 4
MESH = pl.DeviceIdType.MESH
BF16 = jnp.bfloat16
F32 = jnp.float32


def moe_kernel(cfg, tok_in, meta_in, wg, wu, wd, out,
               tok, meta, ring, sib_in, sib_out, own, wbuf, xbuf, hbuf, obuf, ptbuf, sgbuf,
               local_sem, w_sem, ag_s, ag_r, agm_s, agm_r, sb_s, sb_r, sbm_s, sbm_r, own_s, own_r,
               rs_s, rs_r, ss_s, ss_r, credit):
    n, cap, spad, n_w = cfg
    rows, d_model = tok_in.shape
    n_exp, _, d_ff = wg.shape
    chips = n // 2
    far = chips // 2
    half = rows // 2
    piece = half // AG_CHUNKS
    n_d = d_model // COLS
    n_f = d_ff // COLS
    slots = n_exp * spad
    up_loads = 2 * n_exp * n_f
    loads = up_loads + n_d * n_exp // 2
    total_chunks = (far + 1) * n_d
    a_slot, b_slot = 0, far + 1

    me = lax.axis_index('ep')
    chip, core = me // 2, me % 2
    other = 1 - core

    def place(chip_num, core_num):
        return ((chip_num + chips) % chips) * 2 + core_num

    sib = chip * 2 + other
    side = (place(chip + 1, core), place(chip - 1, core))
    sign = (1, -1)

    def load_up(idx, slot, start):
        step = idx // 2
        exp_num, col = step // n_f, pl.multiple_of((step % n_f) * COLS, COLS)
        start(pltpu.make_async_copy(wg.at[exp_num, :, pl.ds(col, COLS)], wbuf.at[slot], w_sem.at[slot, 0]))
        start(pltpu.make_async_copy(wu.at[exp_num, :, pl.ds(col, COLS)], wbuf.at[slot + 1], w_sem.at[slot + 1, 0]))

    def load_down(idx, slot, start):
        col, pair = pl.multiple_of((idx // (n_exp // 2)) * COLS, COLS), idx % (n_exp // 2)
        for k in range(2):
            start(pltpu.make_async_copy(wd.at[pair * 2 + k, :, pl.ds(col, COLS)], wbuf.at[slot, pl.ds(k * d_ff, d_ff)], w_sem.at[slot, k]))

    begin = lambda copy: copy.start()
    finish = lambda copy: copy.wait()

    def part_rows(way, kind, ck):
        upper = (way == 0) == (kind == 1)
        return pl.ds((half if upper else 0) + ck * piece, piece)

    def ag(way, kind, hop, ck, arriving):
        origin = place(chip - sign[way] * (hop if arriving else hop - 1), core)
        if isinstance(ck, int):
            view = tok.at[origin, part_rows(way, kind, ck)]
        else:
            base = half if (way == 0) == (kind == 1) else 0
            view = tok.at[origin, pl.ds(pl.multiple_of(base + ck * piece, piece), piece)]
        copy = pltpu.make_async_remote_copy(view, view, ag_s.at[way, kind, hop - 1, ck], ag_r.at[way, kind, hop - 1, ck], device_id={'ep': side[way]}, device_id_type=MESH)
        return copy, origin, view

    def ag_meta(way, hop, arriving):
        origin = place(chip - sign[way] * (hop if arriving else hop - 1), core)
        view = meta.at[origin]
        copy = pltpu.make_async_remote_copy(view, view, agm_s.at[way, hop - 1], agm_r.at[way, hop - 1], device_id={'ep': side[way]}, device_id_type=MESH)
        return copy, origin, view

    def to_sib(view, send_sem, recv_sem):
        return pltpu.make_async_remote_copy(view, view, send_sem, recv_sem, device_id={'ep': sib}, device_id_type=MESH)

    def sib_view(way, kind, hop, ck, core_num):
        origin = place(chip - sign[way] * hop, core_num)
        base = half if (way == 0) == (kind == 1) else 0
        return tok.at[origin, pl.ds(pl.multiple_of(base + ck * piece, piece), piece)]

    def sib_msg(way, kind, hop, ck, core_num):
        return to_sib(sib_view(way, kind, hop, ck, core_num), sb_s.at[way, kind, hop - 1, ck], sb_r.at[way, kind, hop - 1, ck])

    def sib_meta(way, hop, core_num):
        return to_sib(meta.at[place(chip - sign[way] * hop, core_num)], sbm_s.at[way, hop - 1], sbm_r.at[way, hop - 1])

    meta_hops = (far, far - 1)

    local = (pltpu.make_async_copy(tok_in, tok.at[me], local_sem.at[0]), pltpu.make_async_copy(meta_in, meta.at[me], local_sem.at[1]))
    for copy in local:
        copy.start()
    for idx in range(0, n_w, 2):
        load_up(jnp.int32(idx), idx, begin)
    barrier = pltpu.get_barrier_semaphore()
    for dev in (side[0], side[1], sib):
        pl.semaphore_signal(barrier, inc=1, device_id={'ep': dev}, device_id_type=MESH)
    pl.semaphore_wait(barrier, 3)
    for copy in local:
        copy.wait()

    own_tok = lambda core_num: to_sib(tok.at[place(chip, core_num)], own_s.at[0], own_r.at[0])
    own_meta = lambda core_num: to_sib(meta.at[place(chip, core_num)], own_s.at[1], own_r.at[1])
    for way in range(2):
        ag_meta(way, 1, False)[0].start()
    for ck in range(AG_CHUNKS):
        for way in range(2):
            ag(way, 0, 1, ck, False)[0].start()
    own_meta(core).start()
    own_tok(core).start()
    obuf[...] = jnp.zeros_like(obuf)
    for hop in range(1, far + 1):
        for way in range(2):
            if hop <= meta_hops[way]:
                ag_meta(way, hop, True)[0].wait_recv()
                if hop < meta_hops[way]:
                    ag_meta(way, hop + 1, False)[0].start()
                sib_meta(way, hop, core).start()
        for ck in range(AG_CHUNKS):
            for way in range(2):
                ag(way, 0, hop, ck, True)[0].wait_recv()
                if hop < far:
                    ag(way, 0, hop + 1, ck, False)[0].start()
                sib_msg(way, 0, hop, ck, core).start()
        if hop == far - 1:
            for ck in range(AG_CHUNKS):
                for way in range(2):
                    ag(way, 1, 1, ck, False)[0].start()

    def second_half_event(event):
        hop, ck = event // AG_CHUNKS + 1, event % AG_CHUNKS
        for way in range(2):
            ag(way, 1, hop, ck, True)[0].wait_recv()

            @pl.when(hop < far - 1)
            def _():
                ag(way, 1, hop + 1, ck, False)[0].start()
            sib_msg(way, 1, hop, ck, core).start()

    n_events = (far - 1) * AG_CHUNKS

    def rs(way, slot, d):
        return pltpu.make_async_remote_copy(ring.at[way, slot, d], ring.at[way, slot + 1, d], rs_s.at[way, slot, d], rs_r.at[way, slot + 1, d], device_id={'ep': side[way]}, device_id_type=MESH)

    def rs_wait(way, slot, d):
        pltpu.make_async_remote_copy(ring.at[way, slot, d], ring.at[way, slot, d], rs_s.at[way, slot, d], rs_r.at[way, slot, d], device_id={'ep': side[way]}, device_id_type=MESH).wait_recv()

    lane_rows = (pl.ds(0, half), pl.ds(half, half))

    def phase(dist, order, shards, last=False, events=False):
        width = shards // 2
        m_rows = shards * cap

        def shard_place(num):
            which = num % width
            step = dist if width == 1 else dist * (1 - 2 * which)
            return place(chip + step, jnp.where(num < width, core, other))

        def gather(num, carry):
            shard = shard_place(num)
            base = (me * n_exp * cap).astype(F32)
            row_num = lax.broadcasted_iota(jnp.int32, (slots, rows), 0)
            in_exp = row_num % spad
            want = jnp.where(in_exp < cap, (row_num // spad) * cap + in_exp, -7).astype(F32)
            codes = meta[shard, pl.ds(0, 8), :] - base
            gates = meta[shard, pl.ds(8, 8), :]
            hot = jnp.zeros((slots, rows), F32)
            gate = jnp.zeros((slots, rows), F32)
            for j in range(8):
                same = want == codes[j:j + 1, :]
                hot = jnp.where(same, 1.0, hot)
                gate = jnp.where(same, gates[j:j + 1, :], gate)
            slot_gate = jnp.broadcast_to(jnp.sum(gate, axis=1, keepdims=True), (slots, 128))
            first = pl.multiple_of(num * cap, 16)
            for e in range(n_exp):
                sgbuf[e, pl.ds(first, cap), :] = slot_gate[e * spad:e * spad + cap]
            ptbuf[num] = hot.T.astype(BF16)
            pick = hot.astype(BF16)
            for c in range(d_model // COLS):
                got = jnp.dot(pick, tok[shard, :, pl.ds(c * COLS, COLS)], preferred_element_type=F32).astype(BF16)
                for e in range(n_exp):
                    xbuf[e, pl.ds(first, cap), pl.ds(c * COLS, COLS)] = got[e * spad:e * spad + cap]
            return carry

        lax.fori_loop(0, shards, gather, 0)

        def up_step(step, carry):
            idx = step * 2
            slot = idx % n_w
            load_up(idx, slot, finish)
            e, col = step // n_f, pl.multiple_of((step % n_f) * COLS, COLS)
            x = xbuf[e, pl.ds(0, m_rows), :]
            a = jnp.dot(x, wbuf[slot], preferred_element_type=F32)
            u = jnp.dot(x, wbuf[slot + 1], preferred_element_type=F32)
            hbuf[e, pl.ds(0, m_rows), pl.ds(col, COLS)] = (jax.nn.silu(a) * u).astype(BF16)

            @pl.when(idx + n_w < up_loads)
            def _():
                load_up(idx + n_w, slot, begin)

            @pl.when(idx + n_w >= up_loads)
            def _():
                for k in range(2):
                    load_down(idx + n_w + k - up_loads, slot + k, begin)
            if events:
                every = max(n_exp * n_f // max(n_events - 2, 1), 1)

                @pl.when((step % every == every - 1) & (step // every < n_events - 2))
                def _():
                    second_half_event(step // every)
            return carry

        lax.fori_loop(0, n_exp * n_f, up_step, 0)

        def sib_share(d, waiting=False):
            count = order * n_d + d
            return pltpu.make_async_remote_copy(sib_out.at[d % 2, pl.ds(0, width)], sib_in.at[count % SIB_SLOTS, pl.ds(0, width)], ss_s.at[d % 2], ss_r.at[count % SIB_SLOTS], device_id={'ep': sib}, device_id_type=MESH)

        def close(d):
            count = order * n_d + d
            slot = count % SIB_SLOTS
            sib_share(d).wait_recv()
            mine = lambda i, r: own[d % 2, i, lane_rows[r], :] + sib_in[slot, i, lane_rows[r], :]
            if last:
                for way in range(2):
                    rs_wait(way, a_slot + far, d)
                    rs_wait(way, b_slot + far - 1, d)
                for r in range(2):
                    total = mine(0, r) + ring[r, a_slot + far, d] + ring[1 - r, b_slot + far - 1, d]
                    out[lane_rows[r], pl.ds(pl.multiple_of(d * COLS, COLS), COLS)] = total.astype(BF16)
            elif width == 1:
                for way in range(2):
                    ring[way, a_slot, d] = mine(0, way)
                    rs(way, a_slot, d).start()
            else:
                b_now = b_slot + far - 1 - dist
                a_now = a_slot + far - dist

                @pl.when(dist == far - 1)
                def _():
                    for way in range(2):
                        ring[way, b_slot, d] = mine(way, 1 - way)

                @pl.when(dist != far - 1)
                def _():
                    for way in range(2):
                        rs_wait(way, b_now, d)
                        ring[way, b_now, d] += mine(way, 1 - way)
                for way in range(2):
                    rs(way, b_now, d).start()
                for way in range(2):
                    rs_wait(way, a_now, d)
                    ring[way, a_now, d] += mine(way, way)
                    rs(way, a_now, d).start()

            @pl.when(count < total_chunks - SIB_SLOTS)
            def _():
                pl.semaphore_signal(credit, inc=1, device_id={'ep': sib}, device_id_type=MESH)

        def down_step(d, carry):
            for pair in range(n_exp // 2):
                idx = d * (n_exp // 2) + pair
                slot = (up_loads + idx) % n_w
                load_down(idx, slot, finish)
                for k in range(2):
                    e = pair * 2 + k
                    o = jnp.dot(hbuf[e, pl.ds(0, m_rows), :], wbuf[slot, pl.ds(k * d_ff, d_ff), :], preferred_element_type=F32)
                    g = sgbuf[e, pl.ds(0, m_rows), :]
                    o = o * jnp.concatenate([g] * (COLS // 128), axis=1)
                    for p in range(3):
                        cut = o.astype(BF16)
                        o = o - cut.astype(F32)
                        for i in range(shards):
                            obuf[i, pl.ds(p * slots + e * spad, cap), :] = cut[i * cap:(i + 1) * cap]

                @pl.when(up_loads + idx + n_w < loads)
                def _():
                    load_down(idx + n_w, slot, begin)
                if not last:
                    @pl.when((up_loads + idx + n_w >= loads) & ((up_loads + idx + n_w - loads) % 2 == 1))
                    def _():
                        load_up(up_loads + idx + n_w - loads - 1, slot - 1, begin)

            @pl.when(d >= 2)
            def _():
                sib_share(d).wait_send()

            @pl.when(order * n_d + d >= SIB_SLOTS)
            def _():
                pl.semaphore_wait(credit, 1)
            for i in list(range(width, shards)) + list(range(width)):
                pt = ptbuf[i]
                share = jnp.dot(pt, obuf[i, pl.ds(0, slots), :], preferred_element_type=F32)
                for p in range(1, 3):
                    share += jnp.dot(pt, obuf[i, pl.ds(p * slots, slots), :], preferred_element_type=F32)
                if i >= width:
                    sib_out[d % 2, i - width] = share
                else:
                    own[d % 2, i] = share
                if i == shards - 1:
                    sib_share(d).start()

            @pl.when(d >= 1)
            def _():
                close(d - 1)
            if events:
                for k in range(2):
                    @pl.when(d == (k + 1) * n_d // 2 - 1)
                    def _():
                        second_half_event(n_events - 2 + k)
            return carry

        lax.fori_loop(0, n_d, down_step, 0)
        close(jnp.int32(n_d - 1))
        for d in range(n_d - 2, n_d):
            sib_share(d).wait_send()

    for way in range(2):
        if far <= meta_hops[way]:
            sib_meta(way, far, other).wait_recv()
        for ck in range(AG_CHUNKS):
            sib_msg(way, 0, far, ck, other).wait_recv()
    phase(far, 0, 2, events=True)

    def middle(order, carry):
        dist = far - order
        for way in range(2):
            sib_meta(way, dist, other).wait_recv()
            for kind in range(2):
                for ck in range(AG_CHUNKS):
                    sib_msg(way, kind, dist, ck, other).wait_recv()
        phase(dist, order, 4)
        return carry

    lax.fori_loop(1, far, middle, 0)
    own_meta(other).wait_recv()
    own_tok(other).wait_recv()
    phase(0, far, 2, last=True)

    own_meta(core).wait_send()
    own_tok(core).wait_send()
    for way in range(2):
        for hop in range(1, far + 1):
            if hop <= meta_hops[way]:
                ag_meta(way, hop, False)[0].wait_send()
                sib_meta(way, hop, core).wait_send()
            for kind in range(2):
                if hop <= far - kind:
                    for ck in range(AG_CHUNKS):
                        ag(way, kind, hop, ck, False)[0].wait_send()
                        sib_msg(way, kind, hop, ck, core).wait_send()

        def drain(d, carry):
            for slot in list(range(a_slot, a_slot + far)) + list(range(b_slot, b_slot + far - 1)):
                rs(way, slot, d).wait_send()
            return carry
        lax.fori_loop(0, n_d, drain, 0)


def group_layer(n, tokens, meta, w_gate, w_up, w_down, cap):
    rows, d_model = tokens.shape
    n_exp, _, d_ff = w_gate.shape
    far = n // 4
    spad = (cap + 63) // 64 * 64
    slots = n_exp * spad
    n_d = d_model // COLS
    loads = 2 * n_exp * d_ff // COLS + n_d * n_exp // 2
    n_w = 8 if loads % 8 == 0 else 4
    any_spec = pl.BlockSpec(memory_space=pl.ANY)
    dma = pltpu.SemaphoreType.DMA
    ag_shape = (2, 2, far, AG_CHUNKS)
    return pl.pallas_call(
        functools.partial(moe_kernel, (n, cap, spad, n_w)),
        out_shape=jax.ShapeDtypeStruct((rows, d_model), BF16),
        in_specs=[any_spec] * 5,
        out_specs=pl.BlockSpec(memory_space=pltpu.VMEM),
        scratch_shapes=[
            pltpu.VMEM((n, rows, d_model), BF16),
            pltpu.VMEM((n, 16, rows), F32),
            pltpu.VMEM((2, 2 * far + 1, n_d, rows // 2, COLS), F32),
            pltpu.VMEM((SIB_SLOTS, 2, rows, COLS), F32),
            pltpu.VMEM((2, 2, rows, COLS), F32),
            pltpu.VMEM((2, 2, rows, COLS), F32),
            pltpu.VMEM((n_w, d_model, COLS), BF16),
            pltpu.VMEM((n_exp, 4 * cap, d_model), BF16),
            pltpu.VMEM((n_exp, 4 * cap, d_ff), BF16),
            pltpu.VMEM((4, 3 * slots, COLS), BF16),
            pltpu.VMEM((4, rows, slots), BF16),
            pltpu.VMEM((n_exp, 4 * cap, 128), F32),
            dma((2,)), dma((n_w, 2)),
            dma(ag_shape), dma(ag_shape), dma((2, far)), dma((2, far)),
            dma(ag_shape), dma(ag_shape), dma((2, far)), dma((2, far)),
            dma((2,)), dma((2,)),
            dma((2, 2 * far + 1, n_d)), dma((2, 2 * far + 1, n_d)),
            dma((2,)), dma((SIB_SLOTS,)),
            pltpu.SemaphoreType.REGULAR,
        ],
        compiler_params=pltpu.CompilerParams(collective_id=0, has_side_effects=True, vmem_limit_bytes=67043328),
    )(tokens, meta, w_gate, w_up, w_down)


def solution(mesh):
    group_size = mesh.shape['ep']
    row_spec = P(('dp', 'ep'), None)
    expert_spec = P('ep', None, None)

    def per_device(tokens, expert_ids, gate_wts, slot_ids, w_gate, w_up, w_down):
        rank = lax.axis_index('ep')
        tok_dev, top_k = expert_ids.shape
        cap = CAP_NUM * tok_dev * top_k // (CAP_DEN * w_gate.shape[0] * group_size)
        code = jnp.where(slot_ids >= 0, expert_ids * cap + slot_ids - rank * cap, -1).astype(F32)
        meta = jnp.concatenate([code.T, gate_wts.T], axis=0)
        return group_layer(group_size, tokens, meta, w_gate, w_up, w_down, cap)

    return jax.shard_map(per_device, mesh=mesh, in_specs=(row_spec, row_spec, row_spec, row_spec, expert_spec, expert_spec, expert_spec), out_specs=row_spec, check_vma=False)
```

```python
import functools

import jax
import jax.numpy as jnp
from jax import lax
from jax.experimental import pallas as pl
from jax.experimental.pallas import tpu as pltpu
from jax.sharding import PartitionSpec as P

CAP_NUM = 3
CAP_DEN = 2
COLS = 256
AG_CHUNKS = 2
SIB_SLOTS = 4
MESH = pl.DeviceIdType.MESH
BF16 = jnp.bfloat16
F32 = jnp.float32


def moe_kernel(cfg, tok_in, ids_in, gates_in, slots_in, wg, wu, wd, out,
               tok, meta, raw, ring, sib_in, sib_out, own, wbuf, xbuf, hbuf, obuf, ptbuf, sgbuf,
               local_sem, w_sem, ag_s, ag_r, agm_s, agm_r, sb_s, sb_r, sbm_s, sbm_r, own_s, own_r,
               rs_s, rs_r, ss_s, ss_r, credit):
    n, cap, spad, n_w = cfg
    rows, d_model = tok_in.shape
    top_k = ids_in.shape[0]
    n_exp, _, d_ff = wg.shape
    chips = n // 2
    far = chips // 2
    half = rows // 2
    piece = half // AG_CHUNKS
    n_d = d_model // COLS
    n_f = d_ff // COLS
    slots = n_exp * spad
    up_loads = 2 * n_exp * n_f
    loads = up_loads + n_d * n_exp // 2
    total_chunks = (far + 1) * n_d
    a_slot, b_slot = 0, far + 1

    me = lax.axis_index('ep')
    chip, core = me // 2, me % 2
    other = 1 - core

    def place(chip_num, core_num):
        return ((chip_num + chips) % chips) * 2 + core_num

    sib = chip * 2 + other
    side = (place(chip + 1, core), place(chip - 1, core))
    sign = (1, -1)

    def load_up(idx, slot, start):
        step = idx // 2
        exp_num, col = step // n_f, pl.multiple_of((step % n_f) * COLS, COLS)
        start(pltpu.make_async_copy(wg.at[exp_num, :, pl.ds(col, COLS)], wbuf.at[slot], w_sem.at[slot, 0]))
        start(pltpu.make_async_copy(wu.at[exp_num, :, pl.ds(col, COLS)], wbuf.at[slot + 1], w_sem.at[slot + 1, 0]))

    def load_down(idx, slot, start):
        col, pair = pl.multiple_of((idx // (n_exp // 2)) * COLS, COLS), idx % (n_exp // 2)
        for k in range(2):
            start(pltpu.make_async_copy(wd.at[pair * 2 + k, :, pl.ds(col, COLS)], wbuf.at[slot, pl.ds(k * d_ff, d_ff)], w_sem.at[slot, k]))

    begin = lambda copy: copy.start()
    finish = lambda copy: copy.wait()

    def part_rows(way, kind, ck):
        upper = (way == 0) == (kind == 1)
        return pl.ds((half if upper else 0) + ck * piece, piece)

    def ag(way, kind, hop, ck, arriving):
        origin = place(chip - sign[way] * (hop if arriving else hop - 1), core)
        if isinstance(ck, int):
            view = tok.at[origin, part_rows(way, kind, ck)]
        else:
            base = half if (way == 0) == (kind == 1) else 0
            view = tok.at[origin, pl.ds(pl.multiple_of(base + ck * piece, piece), piece)]
        copy = pltpu.make_async_remote_copy(view, view, ag_s.at[way, kind, hop - 1, ck], ag_r.at[way, kind, hop - 1, ck], device_id={'ep': side[way]}, device_id_type=MESH)
        return copy, origin, view

    def ag_meta(way, hop, arriving):
        origin = place(chip - sign[way] * (hop if arriving else hop - 1), core)
        view = meta.at[origin]
        copy = pltpu.make_async_remote_copy(view, view, agm_s.at[way, hop - 1], agm_r.at[way, hop - 1], device_id={'ep': side[way]}, device_id_type=MESH)
        return copy, origin, view

    def to_sib(view, send_sem, recv_sem):
        return pltpu.make_async_remote_copy(view, view, send_sem, recv_sem, device_id={'ep': sib}, device_id_type=MESH)

    def sib_view(way, kind, hop, ck, core_num):
        origin = place(chip - sign[way] * hop, core_num)
        base = half if (way == 0) == (kind == 1) else 0
        return tok.at[origin, pl.ds(pl.multiple_of(base + ck * piece, piece), piece)]

    def sib_msg(way, kind, hop, ck, core_num):
        return to_sib(sib_view(way, kind, hop, ck, core_num), sb_s.at[way, kind, hop - 1, ck], sb_r.at[way, kind, hop - 1, ck])

    def sib_meta(way, hop, core_num):
        return to_sib(meta.at[place(chip - sign[way] * hop, core_num)], sbm_s.at[way, hop - 1], sbm_r.at[way, hop - 1])

    meta_hops = (far, far - 1)

    barrier = pltpu.get_barrier_semaphore()
    for dev in (side[0], side[1], sib):
        pl.semaphore_signal(barrier, inc=1, device_id={'ep': dev}, device_id_type=MESH)
    local = (pltpu.make_async_copy(ids_in, raw.at[0], local_sem.at[0]), pltpu.make_async_copy(slots_in, raw.at[1], local_sem.at[1]),
             pltpu.make_async_copy(gates_in, meta.at[me, pl.ds(top_k, top_k)], local_sem.at[2]), pltpu.make_async_copy(tok_in, tok.at[me], local_sem.at[3]))
    for copy in local:
        copy.start()
    for copy in local[:2]:
        copy.wait()
    slot_ids = raw[1]
    meta[me, pl.ds(0, top_k), :] = jnp.where(slot_ids >= 0, raw[0] * cap + slot_ids - me * cap, -1).astype(F32)
    for idx in range(0, n_w, 2):
        load_up(jnp.int32(idx), idx, begin)
    for copy in local[2:]:
        copy.wait()
    pl.semaphore_wait(barrier, 3)

    own_tok = lambda core_num: to_sib(tok.at[place(chip, core_num)], own_s.at[0], own_r.at[0])
    own_meta = lambda core_num: to_sib(meta.at[place(chip, core_num)], own_s.at[1], own_r.at[1])
    for way in range(2):
        ag_meta(way, 1, False)[0].start()
    for ck in range(AG_CHUNKS):
        for way in range(2):
            ag(way, 0, 1, ck, False)[0].start()
    own_meta(core).start()
    own_tok(core).start()
    obuf[...] = jnp.zeros_like(obuf)
    for hop in range(1, far + 1):
        for way in range(2):
            if hop <= meta_hops[way]:
                ag_meta(way, hop, True)[0].wait_recv()
                if hop < meta_hops[way]:
                    ag_meta(way, hop + 1, False)[0].start()
                sib_meta(way, hop, core).start()
        for ck in range(AG_CHUNKS):
            for way in range(2):
                ag(way, 0, hop, ck, True)[0].wait_recv()
                if hop < far:
                    ag(way, 0, hop + 1, ck, False)[0].start()
                sib_msg(way, 0, hop, ck, core).start()
        if hop == far - 1:
            for ck in range(AG_CHUNKS):
                for way in range(2):
                    ag(way, 1, 1, ck, False)[0].start()

    def second_half_event(event):
        hop, ck = event // AG_CHUNKS + 1, event % AG_CHUNKS
        for way in range(2):
            ag(way, 1, hop, ck, True)[0].wait_recv()

            @pl.when(hop < far - 1)
            def _():
                ag(way, 1, hop + 1, ck, False)[0].start()
            sib_msg(way, 1, hop, ck, core).start()

    n_events = (far - 1) * AG_CHUNKS

    def rs(way, slot, d):
        return pltpu.make_async_remote_copy(ring.at[way, slot, d], ring.at[way, slot + 1, d], rs_s.at[way, slot, d], rs_r.at[way, slot + 1, d], device_id={'ep': side[way]}, device_id_type=MESH)

    def rs_wait(way, slot, d):
        pltpu.make_async_remote_copy(ring.at[way, slot, d], ring.at[way, slot, d], rs_s.at[way, slot, d], rs_r.at[way, slot, d], device_id={'ep': side[way]}, device_id_type=MESH).wait_recv()

    lane_rows = (pl.ds(0, half), pl.ds(half, half))

    def phase(dist, order, shards, last=False, events=False):
        width = shards // 2
        m_rows = shards * cap

        def shard_place(num):
            which = num % width
            step = dist if width == 1 else dist * (1 - 2 * which)
            return place(chip + step, jnp.where(num < width, core, other))

        def gather(num, carry):
            shard = shard_place(num)
            base = (me * n_exp * cap).astype(F32)
            row_num = lax.broadcasted_iota(jnp.int32, (slots, rows), 0)
            in_exp = row_num % spad
            want = jnp.where(in_exp < cap, (row_num // spad) * cap + in_exp, -7).astype(F32)
            codes = meta[shard, pl.ds(0, top_k), :] - base
            gates = meta[shard, pl.ds(top_k, top_k), :]
            hot = jnp.zeros((slots, rows), F32)
            gate = jnp.zeros((slots, rows), F32)
            for j in range(top_k):
                same = want == codes[j:j + 1, :]
                hot = jnp.where(same, 1.0, hot)
                gate = jnp.where(same, gates[j:j + 1, :], gate)
            slot_gate = jnp.broadcast_to(jnp.sum(gate, axis=1, keepdims=True), (slots, 128))
            first = pl.multiple_of(num * cap, 16)
            for e in range(n_exp):
                sgbuf[e, pl.ds(first, cap), :] = slot_gate[e * spad:e * spad + cap]
            ptbuf[num] = hot.T.astype(BF16)
            pick = hot.astype(BF16)
            for c in range(d_model // COLS):
                got = jnp.dot(pick, tok[shard, :, pl.ds(c * COLS, COLS)], preferred_element_type=F32).astype(BF16)
                for e in range(n_exp):
                    xbuf[e, pl.ds(first, cap), pl.ds(c * COLS, COLS)] = got[e * spad:e * spad + cap]
            return carry

        lax.fori_loop(0, shards, gather, 0)

        def up_step(step, carry):
            idx = step * 2
            slot = idx % n_w
            load_up(idx, slot, finish)
            e, col = step // n_f, pl.multiple_of((step % n_f) * COLS, COLS)
            x = xbuf[e, pl.ds(0, m_rows), :]
            a = jnp.dot(x, wbuf[slot], preferred_element_type=F32)
            u = jnp.dot(x, wbuf[slot + 1], preferred_element_type=F32)
            hbuf[e, pl.ds(0, m_rows), pl.ds(col, COLS)] = (jax.nn.silu(a) * u).astype(BF16)

            @pl.when(idx + n_w < up_loads)
            def _():
                load_up(idx + n_w, slot, begin)

            @pl.when(idx + n_w >= up_loads)
            def _():
                for k in range(2):
                    load_down(idx + n_w + k - up_loads, slot + k, begin)
            if events:
                every = max(n_exp * n_f // max(n_events - 2, 1), 1)

                @pl.when((step % every == every - 1) & (step // every < n_events - 2))
                def _():
                    second_half_event(step // every)
            return carry

        lax.fori_loop(0, n_exp * n_f, up_step, 0)

        def sib_share(d, waiting=False):
            count = order * n_d + d
            return pltpu.make_async_remote_copy(sib_out.at[d % 2, pl.ds(0, width)], sib_in.at[count % SIB_SLOTS, pl.ds(0, width)], ss_s.at[d % 2], ss_r.at[count % SIB_SLOTS], device_id={'ep': sib}, device_id_type=MESH)

        def close(d):
            count = order * n_d + d
            slot = count % SIB_SLOTS
            sib_share(d).wait_recv()
            mine = lambda i, r: own[d % 2, i, lane_rows[r], :] + sib_in[slot, i, lane_rows[r], :]
            if last:
                for way in range(2):
                    rs_wait(way, a_slot + far, d)
                    rs_wait(way, b_slot + far - 1, d)
                for r in range(2):
                    total = mine(0, r) + ring[r, a_slot + far, d] + ring[1 - r, b_slot + far - 1, d]
                    out[lane_rows[r], pl.ds(pl.multiple_of(d * COLS, COLS), COLS)] = total.astype(BF16)
            elif width == 1:
                for way in range(2):
                    ring[way, a_slot, d] = mine(0, way)
                    rs(way, a_slot, d).start()
            else:
                b_now = b_slot + far - 1 - dist
                a_now = a_slot + far - dist

                @pl.when(dist == far - 1)
                def _():
                    for way in range(2):
                        ring[way, b_slot, d] = mine(way, 1 - way)

                @pl.when(dist != far - 1)
                def _():
                    for way in range(2):
                        rs_wait(way, b_now, d)
                        ring[way, b_now, d] += mine(way, 1 - way)
                for way in range(2):
                    rs(way, b_now, d).start()
                for way in range(2):
                    rs_wait(way, a_now, d)
                    ring[way, a_now, d] += mine(way, way)
                    rs(way, a_now, d).start()

            @pl.when(count < total_chunks - SIB_SLOTS)
            def _():
                pl.semaphore_signal(credit, inc=1, device_id={'ep': sib}, device_id_type=MESH)

        def down_step(d, carry):
            for pair in range(n_exp // 2):
                idx = d * (n_exp // 2) + pair
                slot = (up_loads + idx) % n_w
                load_down(idx, slot, finish)
                for k in range(2):
                    e = pair * 2 + k
                    o = jnp.dot(hbuf[e, pl.ds(0, m_rows), :], wbuf[slot, pl.ds(k * d_ff, d_ff), :], preferred_element_type=F32)
                    g = sgbuf[e, pl.ds(0, m_rows), :]
                    o = o * jnp.concatenate([g] * (COLS // 128), axis=1)
                    for p in range(3):
                        cut = o.astype(BF16)
                        o = o - cut.astype(F32)
                        for i in range(shards):
                            obuf[i, pl.ds(p * slots + e * spad, cap), :] = cut[i * cap:(i + 1) * cap]

                @pl.when(up_loads + idx + n_w < loads)
                def _():
                    load_down(idx + n_w, slot, begin)
                if not last:
                    @pl.when((up_loads + idx + n_w >= loads) & ((up_loads + idx + n_w - loads) % 2 == 1))
                    def _():
                        load_up(up_loads + idx + n_w - loads - 1, slot - 1, begin)

            @pl.when(d >= 2)
            def _():
                sib_share(d).wait_send()

            @pl.when(order * n_d + d >= SIB_SLOTS)
            def _():
                pl.semaphore_wait(credit, 1)
            for i in list(range(width, shards)) + list(range(width)):
                pt = ptbuf[i]
                share = jnp.dot(pt, obuf[i, pl.ds(0, slots), :], preferred_element_type=F32)
                for p in range(1, 3):
                    share += jnp.dot(pt, obuf[i, pl.ds(p * slots, slots), :], preferred_element_type=F32)
                if i >= width:
                    sib_out[d % 2, i - width] = share
                else:
                    own[d % 2, i] = share
                if i == shards - 1:
                    sib_share(d).start()

            @pl.when(d >= 1)
            def _():
                close(d - 1)
            if events:
                for k in range(2):
                    @pl.when(d == (k + 1) * n_d // 2 - 1)
                    def _():
                        second_half_event(n_events - 2 + k)
            return carry

        lax.fori_loop(0, n_d, down_step, 0)
        close(jnp.int32(n_d - 1))
        for d in range(n_d - 2, n_d):
            sib_share(d).wait_send()

    for way in range(2):
        if far <= meta_hops[way]:
            sib_meta(way, far, other).wait_recv()
        for ck in range(AG_CHUNKS):
            sib_msg(way, 0, far, ck, other).wait_recv()
    phase(far, 0, 2, events=True)

    def middle(order, carry):
        dist = far - order
        for way in range(2):
            sib_meta(way, dist, other).wait_recv()
            for kind in range(2):
                for ck in range(AG_CHUNKS):
                    sib_msg(way, kind, dist, ck, other).wait_recv()
        phase(dist, order, 4)
        return carry

    lax.fori_loop(1, far, middle, 0)
    own_meta(other).wait_recv()
    own_tok(other).wait_recv()
    phase(0, far, 2, last=True)

    own_meta(core).wait_send()
    own_tok(core).wait_send()
    for way in range(2):
        for hop in range(1, far + 1):
            if hop <= meta_hops[way]:
                ag_meta(way, hop, False)[0].wait_send()
                sib_meta(way, hop, core).wait_send()
            for kind in range(2):
                if hop <= far - kind:
                    for ck in range(AG_CHUNKS):
                        ag(way, kind, hop, ck, False)[0].wait_send()
                        sib_msg(way, kind, hop, ck, core).wait_send()

        def drain(d, carry):
            for slot in list(range(a_slot, a_slot + far)) + list(range(b_slot, b_slot + far - 1)):
                rs(way, slot, d).wait_send()
            return carry
        lax.fori_loop(0, n_d, drain, 0)


def group_layer(n, tokens, ids, gates, slot_ids, w_gate, w_up, w_down, cap):
    rows, d_model = tokens.shape
    top_k = ids.shape[0]
    n_exp, _, d_ff = w_gate.shape
    far = n // 4
    spad = (cap + 63) // 64 * 64
    slots = n_exp * spad
    n_d = d_model // COLS
    loads = 2 * n_exp * d_ff // COLS + n_d * n_exp // 2
    n_w = 8 if loads % 8 == 0 else 4
    any_spec = pl.BlockSpec(memory_space=pl.ANY)
    dma = pltpu.SemaphoreType.DMA
    ag_shape = (2, 2, far, AG_CHUNKS)
    return pl.pallas_call(
        functools.partial(moe_kernel, (n, cap, spad, n_w)),
        out_shape=pltpu.VMEM((rows, d_model), BF16),
        in_specs=[any_spec] * 7,
        out_specs=pl.BlockSpec(memory_space=pltpu.VMEM),
        scratch_shapes=[
            pltpu.VMEM((n, rows, d_model), BF16),
            pltpu.VMEM((n, 2 * top_k, rows), F32),
            pltpu.VMEM((2, top_k, rows), jnp.int32),
            pltpu.VMEM((2, 2 * far + 1, n_d, rows // 2, COLS), F32),
            pltpu.VMEM((SIB_SLOTS, 2, rows, COLS), F32),
            pltpu.VMEM((2, 2, rows, COLS), F32),
            pltpu.VMEM((2, 2, rows, COLS), F32),
            pltpu.VMEM((n_w, d_model, COLS), BF16),
            pltpu.VMEM((n_exp, 4 * cap, d_model), BF16),
            pltpu.VMEM((n_exp, 4 * cap, d_ff), BF16),
            pltpu.VMEM((4, 3 * slots, COLS), BF16),
            pltpu.VMEM((4, rows, slots), BF16),
            pltpu.VMEM((n_exp, 4 * cap, 128), F32),
            dma((4,)), dma((n_w, 2)),
            dma(ag_shape), dma(ag_shape), dma((2, far)), dma((2, far)),
            dma(ag_shape), dma(ag_shape), dma((2, far)), dma((2, far)),
            dma((2,)), dma((2,)),
            dma((2, 2 * far + 1, n_d)), dma((2, 2 * far + 1, n_d)),
            dma((2,)), dma((SIB_SLOTS,)),
            pltpu.SemaphoreType.REGULAR,
        ],
        compiler_params=pltpu.CompilerParams(collective_id=0, has_side_effects=True, vmem_limit_bytes=58 << 20),
    )(tokens, ids, gates, slot_ids, w_gate, w_up, w_down)


def solution(mesh):
    group_size = mesh.shape['ep']
    row_spec = P(('dp', 'ep'), None)
    expert_spec = P('ep', None, None)

    def per_device(tokens, expert_ids, gate_wts, slot_ids, w_gate, w_up, w_down):
        tok_dev, top_k = expert_ids.shape
        cap = CAP_NUM * tok_dev * top_k // (CAP_DEN * w_gate.shape[0] * group_size)
        return group_layer(group_size, tokens, expert_ids.T, gate_wts.T, slot_ids.T, w_gate, w_up, w_down, cap)

    return jax.shard_map(per_device, mesh=mesh, in_specs=(row_spec, row_spec, row_spec, row_spec, expert_spec, expert_spec, expert_spec), out_specs=row_spec, check_vma=False)
```

```python
import functools

import jax
import jax.numpy as jnp
from jax import lax
from jax.experimental import pallas as pl
from jax.experimental.pallas import tpu as pltpu
from jax.sharding import PartitionSpec as P

CAP_NUM = 3
CAP_DEN = 2
COLS = 256
AG_CHUNKS = 2
SIB_SLOTS = 4
PACK = 2
MESH = pl.DeviceIdType.MESH
BF16 = jnp.bfloat16
F32 = jnp.float32


def moe_kernel(cfg, tok_in, ids_in, gates_in, slots_in, wg, wu, wd, out,
               tok, meta, raw, ring, sib_in, sib_out, own, wbuf, xbuf, hbuf, obuf, ptbuf, sgbuf,
               local_sem, w_sem, ag_s, ag_r, agm_s, agm_r, sb_s, sb_r, sbm_s, sbm_r, own_s, own_r,
               rs_s, rs_r, ss_s, ss_r, credit):
    n, cap, spad, n_w = cfg
    rows, d_model = tok_in.shape
    top_k = ids_in.shape[0]
    n_exp, _, d_ff = wg.shape
    chips = n // 2
    far = chips // 2
    half = rows // 2
    piece = half // AG_CHUNKS
    n_d = d_model // COLS
    n_f = d_ff // COLS
    slots = n_exp * spad
    up_loads = 2 * n_exp * n_f
    loads = up_loads + n_d * n_exp // 2
    total_chunks = (far + 1) * n_d
    a_slot, b_slot = 0, far + 1

    me = lax.axis_index('ep')
    chip, core = me // 2, me % 2
    other = 1 - core

    def place(chip_num, core_num):
        return ((chip_num + chips) % chips) * 2 + core_num

    sib = chip * 2 + other
    side = (place(chip + 1, core), place(chip - 1, core))
    sign = (1, -1)

    def load_up(idx, slot, start):
        step = idx // 2
        exp_num, col = step // n_f, pl.multiple_of((step % n_f) * COLS, COLS)
        start(pltpu.make_async_copy(wg.at[exp_num, :, pl.ds(col, COLS)], wbuf.at[slot], w_sem.at[slot, 0]))
        start(pltpu.make_async_copy(wu.at[exp_num, :, pl.ds(col, COLS)], wbuf.at[slot + 1], w_sem.at[slot + 1, 0]))

    def load_down(idx, slot, start):
        col, pair = pl.multiple_of((idx // (n_exp // 2)) * COLS, COLS), idx % (n_exp // 2)
        for k in range(2):
            start(pltpu.make_async_copy(wd.at[pair * 2 + k, :, pl.ds(col, COLS)], wbuf.at[slot, pl.ds(k * d_ff, d_ff)], w_sem.at[slot, k]))

    begin = lambda copy: copy.start()
    finish = lambda copy: copy.wait()

    def part_rows(way, kind, ck):
        upper = (way == 0) == (kind == 1)
        return pl.ds((half if upper else 0) + ck * piece, piece)

    def ag(way, kind, hop, ck, arriving):
        origin = place(chip - sign[way] * (hop if arriving else hop - 1), core)
        if isinstance(ck, int):
            view = tok.at[origin, part_rows(way, kind, ck)]
        else:
            base = half if (way == 0) == (kind == 1) else 0
            view = tok.at[origin, pl.ds(pl.multiple_of(base + ck * piece, piece), piece)]
        copy = pltpu.make_async_remote_copy(view, view, ag_s.at[way, kind, hop - 1, ck], ag_r.at[way, kind, hop - 1, ck], device_id={'ep': side[way]}, device_id_type=MESH)
        return copy, origin, view

    def ag_meta(way, hop, arriving):
        origin = place(chip - sign[way] * (hop if arriving else hop - 1), core)
        view = meta.at[origin]
        copy = pltpu.make_async_remote_copy(view, view, agm_s.at[way, hop - 1], agm_r.at[way, hop - 1], device_id={'ep': side[way]}, device_id_type=MESH)
        return copy, origin, view

    def to_sib(view, send_sem, recv_sem):
        return pltpu.make_async_remote_copy(view, view, send_sem, recv_sem, device_id={'ep': sib}, device_id_type=MESH)

    def sib_view(way, kind, hop, ck, core_num):
        origin = place(chip - sign[way] * hop, core_num)
        base = half if (way == 0) == (kind == 1) else 0
        return tok.at[origin, pl.ds(pl.multiple_of(base + ck * piece, piece), piece)]

    def sib_msg(way, kind, hop, ck, core_num):
        return to_sib(sib_view(way, kind, hop, ck, core_num), sb_s.at[way, kind, hop - 1, ck], sb_r.at[way, kind, hop - 1, ck])

    def sib_meta(way, hop, core_num):
        return to_sib(meta.at[place(chip - sign[way] * hop, core_num)], sbm_s.at[way, hop - 1], sbm_r.at[way, hop - 1])

    meta_hops = (far, far - 1)

    barrier = pltpu.get_barrier_semaphore()
    for dev in (side[0], side[1], sib):
        pl.semaphore_signal(barrier, inc=1, device_id={'ep': dev}, device_id_type=MESH)
    local = (pltpu.make_async_copy(ids_in, raw.at[0], local_sem.at[0]), pltpu.make_async_copy(slots_in, raw.at[1], local_sem.at[1]),
             pltpu.make_async_copy(gates_in, meta.at[me, pl.ds(top_k, top_k)], local_sem.at[2]))
    bands = [pltpu.make_async_copy(tok_in.at[part_rows(way, 0, ck)], tok.at[me, part_rows(way, 0, ck)], local_sem.at[3 + ck * 2 + way]) for ck in range(AG_CHUNKS) for way in range(2)]
    for copy in local + tuple(bands):
        copy.start()
    for copy in local[:2]:
        copy.wait()
    slot_ids = raw[1]
    meta[me, pl.ds(0, top_k), :] = jnp.where(slot_ids >= 0, raw[0] * cap + slot_ids - me * cap, -1).astype(F32)
    for idx in range(0, n_w, 2):
        load_up(jnp.int32(idx), idx, begin)
    pl.semaphore_wait(barrier, 3)

    own_tok = lambda core_num: to_sib(tok.at[place(chip, core_num)], own_s.at[0], own_r.at[0])
    own_meta = lambda core_num: to_sib(meta.at[place(chip, core_num)], own_s.at[1], own_r.at[1])
    for ck in range(AG_CHUNKS):
        for way in range(2):
            bands[ck * 2 + way].wait()
            ag(way, 0, 1, ck, False)[0].start()
        if ck == 0:
            local[2].wait()
            for way in range(2):
                ag_meta(way, 1, False)[0].start()
    own_meta(core).start()
    own_tok(core).start()
    obuf[...] = jnp.zeros_like(obuf)
    for hop in range(1, far + 1):
        for ck in range(AG_CHUNKS):
            for way in range(2):
                ag(way, 0, hop, ck, True)[0].wait_recv()
                if hop < far:
                    ag(way, 0, hop + 1, ck, False)[0].start()
                sib_msg(way, 0, hop, ck, core).start()
                if ck == 0 and hop <= meta_hops[way]:
                    ag_meta(way, hop, True)[0].wait_recv()
                    if hop < meta_hops[way]:
                        ag_meta(way, hop + 1, False)[0].start()
                    sib_meta(way, hop, core).start()
        if hop == far - 1:
            for ck in range(AG_CHUNKS):
                for way in range(2):
                    ag(way, 1, 1, ck, False)[0].start()

    def second_half_event(event):
        hop, ck = event // AG_CHUNKS + 1, event % AG_CHUNKS
        for way in range(2):
            ag(way, 1, hop, ck, True)[0].wait_recv()

            @pl.when(hop < far - 1)
            def _():
                ag(way, 1, hop + 1, ck, False)[0].start()
            sib_msg(way, 1, hop, ck, core).start()

    n_events = (far - 1) * AG_CHUNKS

    def rs(way, slot, d):
        return pltpu.make_async_remote_copy(ring.at[way, slot, d], ring.at[way, slot + 1, d], rs_s.at[way, slot, d], rs_r.at[way, slot + 1, d], device_id={'ep': side[way]}, device_id_type=MESH)

    def rs_wait(way, slot, d):
        @pl.when(d % PACK == 0)
        def _():
            rs_arrived(way, slot, d // PACK)

    def rs_send(way, slot, d):
        @pl.when(d % PACK == PACK - 1)
        def _():
            rs(way, slot, d // PACK).start()

    def rs_arrived(way, slot, d):
        pltpu.make_async_remote_copy(ring.at[way, slot, d], ring.at[way, slot, d], rs_s.at[way, slot, d], rs_r.at[way, slot, d], device_id={'ep': side[way]}, device_id_type=MESH).wait_recv()

    lane_rows = (pl.ds(0, half), pl.ds(half, half))

    def phase(dist, order, shards, last=False, events=False):
        width = shards // 2
        m_rows = shards * cap

        def shard_place(num):
            which = num % width
            step = dist if width == 1 else dist * (1 - 2 * which)
            return place(chip + step, jnp.where(num < width, core, other))

        def gather(num, carry):
            shard = shard_place(num)
            base = (me * n_exp * cap).astype(F32)
            row_num = lax.broadcasted_iota(jnp.int32, (slots, rows), 0)
            in_exp = row_num % spad
            want = jnp.where(in_exp < cap, (row_num // spad) * cap + in_exp, -7).astype(F32)
            codes = meta[shard, pl.ds(0, top_k), :] - base
            gates = meta[shard, pl.ds(top_k, top_k), :]
            hot = jnp.zeros((slots, rows), F32)
            gate = jnp.zeros((slots, rows), F32)
            for j in range(top_k):
                same = want == codes[j:j + 1, :]
                hot = jnp.where(same, 1.0, hot)
                gate = jnp.where(same, gates[j:j + 1, :], gate)
            slot_gate = jnp.broadcast_to(jnp.sum(gate, axis=1, keepdims=True), (slots, 128))
            first = pl.multiple_of(num * cap, 16)
            for e in range(n_exp):
                sgbuf[e, pl.ds(first, cap), :] = slot_gate[e * spad:e * spad + cap]
            ptbuf[num] = hot.T.astype(BF16)
            pick = hot.astype(BF16)
            for c in range(d_model // COLS):
                got = jnp.dot(pick, tok[shard, :, pl.ds(c * COLS, COLS)], preferred_element_type=F32).astype(BF16)
                for e in range(n_exp):
                    xbuf[e, pl.ds(first, cap), pl.ds(c * COLS, COLS)] = got[e * spad:e * spad + cap]
            return carry

        lax.fori_loop(0, shards, gather, 0)

        def up_step(step, carry):
            idx = step * 2
            slot = idx % n_w
            load_up(idx, slot, finish)
            e, col = step // n_f, pl.multiple_of((step % n_f) * COLS, COLS)
            x = xbuf[e, pl.ds(0, m_rows), :]
            a = jnp.dot(x, wbuf[slot], preferred_element_type=F32)
            u = jnp.dot(x, wbuf[slot + 1], preferred_element_type=F32)
            hbuf[e, pl.ds(0, m_rows), pl.ds(col, COLS)] = (jax.nn.silu(a) * u).astype(BF16)

            @pl.when(idx + n_w < up_loads)
            def _():
                load_up(idx + n_w, slot, begin)

            @pl.when(idx + n_w >= up_loads)
            def _():
                for k in range(2):
                    load_down(idx + n_w + k - up_loads, slot + k, begin)
            if events:
                every = max(n_exp * n_f // max(n_events - 2, 1), 1)

                @pl.when((step % every == every - 1) & (step // every < n_events - 2))
                def _():
                    second_half_event(step // every)
            return carry

        lax.fori_loop(0, n_exp * n_f, up_step, 0)

        def sib_share(d, waiting=False):
            count = order * n_d + d
            return pltpu.make_async_remote_copy(sib_out.at[d % 2, pl.ds(0, width)], sib_in.at[count % SIB_SLOTS, pl.ds(0, width)], ss_s.at[d % 2], ss_r.at[count % SIB_SLOTS], device_id={'ep': sib}, device_id_type=MESH)

        def close(d):
            count = order * n_d + d
            slot = count % SIB_SLOTS
            sib_share(d).wait_recv()
            mine = lambda i, r: own[d % 2, i, lane_rows[r], :] + sib_in[slot, i, lane_rows[r], :]
            if last:
                for way in range(2):
                    rs_wait(way, a_slot + far, d)
                    rs_wait(way, b_slot + far - 1, d)
                for r in range(2):
                    total = mine(0, r) + ring[r, a_slot + far, d // PACK, d % PACK] + ring[1 - r, b_slot + far - 1, d // PACK, d % PACK]
                    out[lane_rows[r], pl.ds(pl.multiple_of(d * COLS, COLS), COLS)] = total.astype(BF16)
            elif width == 1:
                for way in range(2):
                    ring[way, a_slot, d // PACK, d % PACK] = mine(0, way)
                    rs_send(way, a_slot, d)
            else:
                b_now = b_slot + far - 1 - dist
                a_now = a_slot + far - dist

                @pl.when(dist == far - 1)
                def _():
                    for way in range(2):
                        ring[way, b_slot, d // PACK, d % PACK] = mine(way, 1 - way)

                @pl.when(dist != far - 1)
                def _():
                    for way in range(2):
                        rs_wait(way, b_now, d)
                        ring[way, b_now, d // PACK, d % PACK] += mine(way, 1 - way)
                for way in range(2):
                    rs_send(way, b_now, d)
                for way in range(2):
                    rs_wait(way, a_now, d)
                    ring[way, a_now, d // PACK, d % PACK] += mine(way, way)
                    rs_send(way, a_now, d)

            @pl.when(count < total_chunks - SIB_SLOTS)
            def _():
                pl.semaphore_signal(credit, inc=1, device_id={'ep': sib}, device_id_type=MESH)

        def down_step(d, carry):
            for pair in range(n_exp // 2):
                idx = d * (n_exp // 2) + pair
                slot = (up_loads + idx) % n_w
                load_down(idx, slot, finish)
                for k in range(2):
                    e = pair * 2 + k
                    o = jnp.dot(hbuf[e, pl.ds(0, m_rows), :], wbuf[slot, pl.ds(k * d_ff, d_ff), :], preferred_element_type=F32)
                    g = sgbuf[e, pl.ds(0, m_rows), :]
                    o = o * jnp.concatenate([g] * (COLS // 128), axis=1)
                    for p in range(3):
                        cut = o.astype(BF16)
                        o = o - cut.astype(F32)
                        for i in range(shards):
                            obuf[i, pl.ds(p * slots + e * spad, cap), :] = cut[i * cap:(i + 1) * cap]

                @pl.when(up_loads + idx + n_w < loads)
                def _():
                    load_down(idx + n_w, slot, begin)
                if not last:
                    @pl.when((up_loads + idx + n_w >= loads) & ((up_loads + idx + n_w - loads) % 2 == 1))
                    def _():
                        load_up(up_loads + idx + n_w - loads - 1, slot - 1, begin)

            @pl.when(d >= 2)
            def _():
                sib_share(d).wait_send()

            @pl.when(order * n_d + d >= SIB_SLOTS)
            def _():
                pl.semaphore_wait(credit, 1)
            for i in list(range(width, shards)) + list(range(width)):
                pt = ptbuf[i]
                share = jnp.dot(pt, obuf[i, pl.ds(0, slots), :], preferred_element_type=F32)
                for p in range(1, 3):
                    share += jnp.dot(pt, obuf[i, pl.ds(p * slots, slots), :], preferred_element_type=F32)
                if i >= width:
                    sib_out[d % 2, i - width] = share
                else:
                    own[d % 2, i] = share
                if i == shards - 1:
                    sib_share(d).start()

            @pl.when(d >= 1)
            def _():
                close(d - 1)
            if events:
                for k in range(2):
                    @pl.when(d == (k + 1) * n_d // 2 - 1)
                    def _():
                        second_half_event(n_events - 2 + k)
            return carry

        lax.fori_loop(0, n_d, down_step, 0)
        close(jnp.int32(n_d - 1))
        for d in range(n_d - 2, n_d):
            sib_share(d).wait_send()

    for way in range(2):
        if far <= meta_hops[way]:
            sib_meta(way, far, other).wait_recv()
        for ck in range(AG_CHUNKS):
            sib_msg(way, 0, far, ck, other).wait_recv()
    phase(far, 0, 2, events=True)

    def middle(order, carry):
        dist = far - order
        for way in range(2):
            sib_meta(way, dist, other).wait_recv()
            for kind in range(2):
                for ck in range(AG_CHUNKS):
                    sib_msg(way, kind, dist, ck, other).wait_recv()
        phase(dist, order, 4)
        return carry

    lax.fori_loop(1, far, middle, 0)
    own_meta(other).wait_recv()
    own_tok(other).wait_recv()
    phase(0, far, 2, last=True)

    own_meta(core).wait_send()
    own_tok(core).wait_send()
    for way in range(2):
        for hop in range(1, far + 1):
            if hop <= meta_hops[way]:
                ag_meta(way, hop, False)[0].wait_send()
                sib_meta(way, hop, core).wait_send()
            for kind in range(2):
                if hop <= far - kind:
                    for ck in range(AG_CHUNKS):
                        ag(way, kind, hop, ck, False)[0].wait_send()
                        sib_msg(way, kind, hop, ck, core).wait_send()

        def drain(d, carry):
            for slot in list(range(a_slot, a_slot + far)) + list(range(b_slot, b_slot + far - 1)):
                rs(way, slot, d).wait_send()
            return carry
        lax.fori_loop(0, n_d // PACK, drain, 0)


def group_layer(n, tokens, ids, gates, slot_ids, w_gate, w_up, w_down, cap):
    rows, d_model = tokens.shape
    top_k = ids.shape[0]
    n_exp, _, d_ff = w_gate.shape
    far = n // 4
    spad = (cap + 63) // 64 * 64
    slots = n_exp * spad
    n_d = d_model // COLS
    loads = 2 * n_exp * d_ff // COLS + n_d * n_exp // 2
    n_w = 8 if loads % 8 == 0 else 4
    any_spec = pl.BlockSpec(memory_space=pl.ANY)
    dma = pltpu.SemaphoreType.DMA
    ag_shape = (2, 2, far, AG_CHUNKS)
    return pl.pallas_call(
        functools.partial(moe_kernel, (n, cap, spad, n_w)),
        out_shape=pltpu.VMEM((rows, d_model), BF16),
        in_specs=[any_spec] * 7,
        out_specs=pl.BlockSpec(memory_space=pltpu.VMEM),
        scratch_shapes=[
            pltpu.VMEM((n, rows, d_model), BF16),
            pltpu.VMEM((n, 2 * top_k, rows), F32),
            pltpu.VMEM((2, top_k, rows), jnp.int32),
            pltpu.VMEM((2, 2 * far + 1, n_d // PACK, PACK, rows // 2, COLS), F32),
            pltpu.VMEM((SIB_SLOTS, 2, rows, COLS), F32),
            pltpu.VMEM((2, 2, rows, COLS), F32),
            pltpu.VMEM((2, 2, rows, COLS), F32),
            pltpu.VMEM((n_w, d_model, COLS), BF16),
            pltpu.VMEM((n_exp, 4 * cap, d_model), BF16),
            pltpu.VMEM((n_exp, 4 * cap, d_ff), BF16),
            pltpu.VMEM((4, 3 * slots, COLS), BF16),
            pltpu.VMEM((4, rows, slots), BF16),
            pltpu.VMEM((n_exp, 4 * cap, 128), F32),
            dma((3 + 2 * AG_CHUNKS,)), dma((n_w, 2)),
            dma(ag_shape), dma(ag_shape), dma((2, far)), dma((2, far)),
            dma(ag_shape), dma(ag_shape), dma((2, far)), dma((2, far)),
            dma((2,)), dma((2,)),
            dma((2, 2 * far + 1, n_d // PACK)), dma((2, 2 * far + 1, n_d // PACK)),
            dma((2,)), dma((SIB_SLOTS,)),
            pltpu.SemaphoreType.REGULAR,
        ],
        compiler_params=pltpu.CompilerParams(collective_id=0, has_side_effects=True, vmem_limit_bytes=58 << 20),
    )(tokens, ids, gates, slot_ids, w_gate, w_up, w_down)


def solution(mesh):
    group_size = mesh.shape['ep']
    row_spec = P(('dp', 'ep'), None)
    expert_spec = P('ep', None, None)

    def per_device(tokens, expert_ids, gate_wts, slot_ids, w_gate, w_up, w_down):
        tok_dev, top_k = expert_ids.shape
        cap = CAP_NUM * tok_dev * top_k // (CAP_DEN * w_gate.shape[0] * group_size)
        return group_layer(group_size, tokens, expert_ids.T, gate_wts.T, slot_ids.T, w_gate, w_up, w_down, cap)

    return jax.shard_map(per_device, mesh=mesh, in_specs=(row_spec, row_spec, row_spec, row_spec, expert_spec, expert_spec, expert_spec), out_specs=row_spec, check_vma=False)
```

```python
import functools

import jax
import jax.numpy as jnp
from jax import lax
from jax.experimental import pallas as pl
from jax.experimental.pallas import tpu as pltpu
from jax.sharding import PartitionSpec as P

CAP_NUM = 3
CAP_DEN = 2
COLS = 256
AG_CHUNKS = 2
SIB_SLOTS = 4
PACK = 2
MESH = pl.DeviceIdType.MESH
BF16 = jnp.bfloat16
F32 = jnp.float32


def moe_kernel(cfg, tok_in, ids_in, gates_in, slots_in, wg, wu, wd, out,
               tok, meta, raw, ring, sib_in, sib_out, own, wbuf, xbuf, hbuf, obuf, ptbuf, pbuf, sgbuf,
               local_sem, w_sem, ag_s, ag_r, agm_s, agm_r, sb_s, sb_r, sbm_s, sbm_r, own_s, own_r,
               rs_s, rs_r, ss_s, ss_r, credit):
    n, cap, spad, n_w = cfg
    rows, d_model = tok_in.shape
    top_k = ids_in.shape[0]
    n_exp, _, d_ff = wg.shape
    chips = n // 2
    far = chips // 2
    half = rows // 2
    piece = half // AG_CHUNKS
    n_d = d_model // COLS
    n_f = d_ff // COLS
    slots = n_exp * spad
    up_loads = 2 * n_exp * n_f
    loads = up_loads + n_d * n_exp // 2
    total_chunks = (far + 1) * n_d
    a_slot, b_slot = 0, far + 1

    me = lax.axis_index('ep')
    chip, core = me // 2, me % 2
    other = 1 - core

    def place(chip_num, core_num):
        return ((chip_num + chips) % chips) * 2 + core_num

    sib = chip * 2 + other
    side = (place(chip + 1, core), place(chip - 1, core))
    sign = (1, -1)

    def load_up(idx, slot, start):
        step = idx // 2
        exp_num, col = step // n_f, pl.multiple_of((step % n_f) * COLS, COLS)
        start(pltpu.make_async_copy(wg.at[exp_num, :, pl.ds(col, COLS)], wbuf.at[slot], w_sem.at[slot, 0]))
        start(pltpu.make_async_copy(wu.at[exp_num, :, pl.ds(col, COLS)], wbuf.at[slot + 1], w_sem.at[slot + 1, 0]))

    def load_down(idx, slot, start):
        col, pair = pl.multiple_of((idx // (n_exp // 2)) * COLS, COLS), idx % (n_exp // 2)
        for k in range(2):
            start(pltpu.make_async_copy(wd.at[pair * 2 + k, :, pl.ds(col, COLS)], wbuf.at[slot, pl.ds(k * d_ff, d_ff)], w_sem.at[slot, k]))

    begin = lambda copy: copy.start()
    finish = lambda copy: copy.wait()

    def part_rows(way, kind, ck):
        upper = (way == 0) == (kind == 1)
        return pl.ds((half if upper else 0) + ck * piece, piece)

    def ag(way, kind, hop, ck, arriving):
        origin = place(chip - sign[way] * (hop if arriving else hop - 1), core)
        if isinstance(ck, int):
            view = tok.at[origin, part_rows(way, kind, ck)]
        else:
            base = half if (way == 0) == (kind == 1) else 0
            view = tok.at[origin, pl.ds(pl.multiple_of(base + ck * piece, piece), piece)]
        copy = pltpu.make_async_remote_copy(view, view, ag_s.at[way, kind, hop - 1, ck], ag_r.at[way, kind, hop - 1, ck], device_id={'ep': side[way]}, device_id_type=MESH)
        return copy, origin, view

    def ag_meta(way, hop, arriving):
        origin = place(chip - sign[way] * (hop if arriving else hop - 1), core)
        view = meta.at[origin]
        copy = pltpu.make_async_remote_copy(view, view, agm_s.at[way, hop - 1], agm_r.at[way, hop - 1], device_id={'ep': side[way]}, device_id_type=MESH)
        return copy, origin, view

    def to_sib(view, send_sem, recv_sem):
        return pltpu.make_async_remote_copy(view, view, send_sem, recv_sem, device_id={'ep': sib}, device_id_type=MESH)

    def sib_view(way, kind, hop, ck, core_num):
        origin = place(chip - sign[way] * hop, core_num)
        base = half if (way == 0) == (kind == 1) else 0
        return tok.at[origin, pl.ds(pl.multiple_of(base + ck * piece, piece), piece)]

    def sib_msg(way, kind, hop, ck, core_num):
        return to_sib(sib_view(way, kind, hop, ck, core_num), sb_s.at[way, kind, hop - 1, ck], sb_r.at[way, kind, hop - 1, ck])

    def sib_meta(way, hop, core_num):
        return to_sib(meta.at[place(chip - sign[way] * hop, core_num)], sbm_s.at[way, hop - 1], sbm_r.at[way, hop - 1])

    meta_hops = (far, far - 1)

    barrier = pltpu.get_barrier_semaphore()
    for dev in (side[0], side[1], sib):
        pl.semaphore_signal(barrier, inc=1, device_id={'ep': dev}, device_id_type=MESH)
    local = (pltpu.make_async_copy(ids_in, raw.at[0], local_sem.at[0]), pltpu.make_async_copy(slots_in, raw.at[1], local_sem.at[1]),
             pltpu.make_async_copy(gates_in, meta.at[me, pl.ds(top_k, top_k)], local_sem.at[2]))
    bands = [pltpu.make_async_copy(tok_in.at[part_rows(way, 0, ck)], tok.at[me, part_rows(way, 0, ck)], local_sem.at[3 + ck * 2 + way]) for ck in range(AG_CHUNKS) for way in range(2)]
    for copy in local + tuple(bands):
        copy.start()
    for copy in local[:2]:
        copy.wait()
    slot_ids = raw[1]
    meta[me, pl.ds(0, top_k), :] = jnp.where(slot_ids >= 0, raw[0] * cap + slot_ids - me * cap, -1).astype(F32)
    for idx in range(0, n_w, 2):
        load_up(jnp.int32(idx), idx, begin)
    pl.semaphore_wait(barrier, 3)

    own_tok = lambda core_num: to_sib(tok.at[place(chip, core_num)], own_s.at[0], own_r.at[0])
    own_meta = lambda core_num: to_sib(meta.at[place(chip, core_num)], own_s.at[1], own_r.at[1])
    for ck in range(AG_CHUNKS):
        for way in range(2):
            bands[ck * 2 + way].wait()
            ag(way, 0, 1, ck, False)[0].start()
        if ck == 0:
            local[2].wait()
            for way in range(2):
                ag_meta(way, 1, False)[0].start()
    own_meta(core).start()
    own_tok(core).start()
    obuf[...] = jnp.zeros_like(obuf)
    for hop in range(1, far + 1):
        for ck in range(AG_CHUNKS):
            for way in range(2):
                ag(way, 0, hop, ck, True)[0].wait_recv()
                if hop < far:
                    ag(way, 0, hop + 1, ck, False)[0].start()
                sib_msg(way, 0, hop, ck, core).start()
                if ck == 0 and hop <= meta_hops[way]:
                    ag_meta(way, hop, True)[0].wait_recv()
                    if hop < meta_hops[way]:
                        ag_meta(way, hop + 1, False)[0].start()
                    sib_meta(way, hop, core).start()
        if hop == far - 1:
            for ck in range(AG_CHUNKS):
                for way in range(2):
                    ag(way, 1, 1, ck, False)[0].start()

    def second_half_event(event):
        hop, ck = event // AG_CHUNKS + 1, event % AG_CHUNKS
        for way in range(2):
            ag(way, 1, hop, ck, True)[0].wait_recv()

            @pl.when(hop < far - 1)
            def _():
                ag(way, 1, hop + 1, ck, False)[0].start()
            sib_msg(way, 1, hop, ck, core).start()

    n_events = (far - 1) * AG_CHUNKS

    def rs(way, slot, d):
        return pltpu.make_async_remote_copy(ring.at[way, slot, d], ring.at[way, slot + 1, d], rs_s.at[way, slot, d], rs_r.at[way, slot + 1, d], device_id={'ep': side[way]}, device_id_type=MESH)

    def rs_wait(way, slot, d):
        @pl.when(d % PACK == 0)
        def _():
            rs_arrived(way, slot, d // PACK)

    def rs_send(way, slot, d):
        @pl.when(d % PACK == PACK - 1)
        def _():
            rs(way, slot, d // PACK).start()

    def rs_arrived(way, slot, d):
        pltpu.make_async_remote_copy(ring.at[way, slot, d], ring.at[way, slot, d], rs_s.at[way, slot, d], rs_r.at[way, slot, d], device_id={'ep': side[way]}, device_id_type=MESH).wait_recv()

    lane_rows = (pl.ds(0, half), pl.ds(half, half))

    def phase(dist, order, shards, arrive, last=False, events=False):
        width = shards // 2
        m_rows = shards * cap

        def shard_place(num):
            which = num % width
            step = dist if width == 1 else dist * (1 - 2 * which)
            return place(chip + step, jnp.where(num < width, core, other))

        def masks(num, carry):
            shard = shard_place(num)
            base = (me * n_exp * cap).astype(F32)
            row_num = lax.broadcasted_iota(jnp.int32, (slots, rows), 0)
            in_exp = row_num % spad
            want = jnp.where(in_exp < cap, (row_num // spad) * cap + in_exp, -7).astype(F32)
            codes = meta[shard, pl.ds(0, top_k), :] - base
            gates = meta[shard, pl.ds(top_k, top_k), :]
            hot = jnp.zeros((slots, rows), F32)
            gate = jnp.zeros((slots, rows), F32)
            for j in range(top_k):
                same = want == codes[j:j + 1, :]
                hot = jnp.where(same, 1.0, hot)
                gate = jnp.where(same, gates[j:j + 1, :], gate)
            slot_gate = jnp.broadcast_to(jnp.sum(gate, axis=1, keepdims=True), (slots, 128))
            first = pl.multiple_of(num * cap, 16)
            for e in range(n_exp):
                sgbuf[e, pl.ds(first, cap), :] = slot_gate[e * spad:e * spad + cap]
            ptbuf[num] = hot.T.astype(BF16)
            pbuf[num] = hot.astype(BF16)
            return carry

        def gather(num, carry):
            shard = shard_place(num)
            first = pl.multiple_of(num * cap, 16)
            pick = pbuf[num]
            for c in range(d_model // COLS):
                got = jnp.dot(pick, tok[shard, :, pl.ds(c * COLS, COLS)], preferred_element_type=F32).astype(BF16)
                for e in range(n_exp):
                    xbuf[e, pl.ds(first, cap), pl.ds(c * COLS, COLS)] = got[e * spad:e * spad + cap]
            return carry

        lax.fori_loop(0, shards, masks, 0)
        arrive()
        lax.fori_loop(0, shards, gather, 0)

        def up_step(step, carry):
            idx = step * 2
            slot = idx % n_w
            load_up(idx, slot, finish)
            e, col = step // n_f, pl.multiple_of((step % n_f) * COLS, COLS)
            x = xbuf[e, pl.ds(0, m_rows), :]
            a = jnp.dot(x, wbuf[slot], preferred_element_type=F32)
            u = jnp.dot(x, wbuf[slot + 1], preferred_element_type=F32)
            hbuf[e, pl.ds(0, m_rows), pl.ds(col, COLS)] = (jax.nn.silu(a) * u).astype(BF16)

            @pl.when(idx + n_w < up_loads)
            def _():
                load_up(idx + n_w, slot, begin)

            @pl.when(idx + n_w >= up_loads)
            def _():
                for k in range(2):
                    load_down(idx + n_w + k - up_loads, slot + k, begin)
            if events:
                every = max(n_exp * n_f // max(n_events - 2, 1), 1)

                @pl.when((step % every == every - 1) & (step // every < n_events - 2))
                def _():
                    second_half_event(step // every)
            return carry

        lax.fori_loop(0, n_exp * n_f, up_step, 0)

        def sib_share(d, waiting=False):
            count = order * n_d + d
            return pltpu.make_async_remote_copy(sib_out.at[d % 2, pl.ds(0, width)], sib_in.at[count % SIB_SLOTS, pl.ds(0, width)], ss_s.at[d % 2], ss_r.at[count % SIB_SLOTS], device_id={'ep': sib}, device_id_type=MESH)

        def close(d):
            count = order * n_d + d
            slot = count % SIB_SLOTS
            sib_share(d).wait_recv()
            mine = lambda i, r: own[d % 2, i, lane_rows[r], :] + sib_in[slot, i, lane_rows[r], :]
            if last:
                for way in range(2):
                    rs_wait(way, a_slot + far, d)
                    rs_wait(way, b_slot + far - 1, d)
                for r in range(2):
                    total = mine(0, r) + ring[r, a_slot + far, d // PACK, d % PACK] + ring[1 - r, b_slot + far - 1, d // PACK, d % PACK]
                    out[lane_rows[r], pl.ds(pl.multiple_of(d * COLS, COLS), COLS)] = total.astype(BF16)
            elif width == 1:
                for way in range(2):
                    ring[way, a_slot, d // PACK, d % PACK] = mine(0, way)
                    rs_send(way, a_slot, d)
            else:
                b_now = b_slot + far - 1 - dist
                a_now = a_slot + far - dist

                @pl.when(dist == far - 1)
                def _():
                    for way in range(2):
                        ring[way, b_slot, d // PACK, d % PACK] = mine(way, 1 - way)

                @pl.when(dist != far - 1)
                def _():
                    for way in range(2):
                        rs_wait(way, b_now, d)
                        ring[way, b_now, d // PACK, d % PACK] += mine(way, 1 - way)
                for way in range(2):
                    rs_send(way, b_now, d)
                for way in range(2):
                    rs_wait(way, a_now, d)
                    ring[way, a_now, d // PACK, d % PACK] += mine(way, way)
                    rs_send(way, a_now, d)

            @pl.when(count < total_chunks - SIB_SLOTS)
            def _():
                pl.semaphore_signal(credit, inc=1, device_id={'ep': sib}, device_id_type=MESH)

        def down_step(d, carry):
            for pair in range(n_exp // 2):
                idx = d * (n_exp // 2) + pair
                slot = (up_loads + idx) % n_w
                load_down(idx, slot, finish)
                for k in range(2):
                    e = pair * 2 + k
                    o = jnp.dot(hbuf[e, pl.ds(0, m_rows), :], wbuf[slot, pl.ds(k * d_ff, d_ff), :], preferred_element_type=F32)
                    g = sgbuf[e, pl.ds(0, m_rows), :]
                    o = o * jnp.concatenate([g] * (COLS // 128), axis=1)
                    for p in range(3):
                        cut = o.astype(BF16)
                        o = o - cut.astype(F32)
                        for i in range(shards):
                            obuf[i, pl.ds(p * slots + e * spad, cap), :] = cut[i * cap:(i + 1) * cap]

                @pl.when(up_loads + idx + n_w < loads)
                def _():
                    load_down(idx + n_w, slot, begin)
                if not last:
                    @pl.when((up_loads + idx + n_w >= loads) & ((up_loads + idx + n_w - loads) % 2 == 1))
                    def _():
                        load_up(up_loads + idx + n_w - loads - 1, slot - 1, begin)

            @pl.when(d >= 2)
            def _():
                sib_share(d).wait_send()

            @pl.when(order * n_d + d >= SIB_SLOTS)
            def _():
                pl.semaphore_wait(credit, 1)
            for i in list(range(width, shards)) + list(range(width)):
                pt = ptbuf[i]
                share = jnp.dot(pt, obuf[i, pl.ds(0, slots), :], preferred_element_type=F32)
                for p in range(1, 3):
                    share += jnp.dot(pt, obuf[i, pl.ds(p * slots, slots), :], preferred_element_type=F32)
                if i >= width:
                    sib_out[d % 2, i - width] = share
                else:
                    own[d % 2, i] = share
                if i == shards - 1:
                    sib_share(d).start()

            @pl.when(d >= 1)
            def _():
                close(d - 1)
            if events:
                @pl.when(d == n_d // 2 - 1)
                def _():
                    second_half_event(n_events - 2)
            return carry

        lax.fori_loop(0, n_d, down_step, 0)
        close(jnp.int32(n_d - 1))
        for d in range(n_d - 2, n_d):
            sib_share(d).wait_send()

    def far_rows():
        for way in range(2):
            for ck in range(AG_CHUNKS):
                sib_msg(way, 0, far, ck, other).wait_recv()

    for way in range(2):
        if far <= meta_hops[way]:
            sib_meta(way, far, other).wait_recv()
    phase(far, 0, 2, far_rows, events=True)

    def middle(order, carry):
        dist = far - order

        def rows_of():
            @pl.when(order == 1)
            def _():
                second_half_event(n_events - 1)
            for way in range(2):
                for kind in range(2):
                    for ck in range(AG_CHUNKS):
                        sib_msg(way, kind, dist, ck, other).wait_recv()

        for way in range(2):
            sib_meta(way, dist, other).wait_recv()
        phase(dist, order, 4, rows_of)
        return carry

    lax.fori_loop(1, far, middle, 0)
    own_meta(other).wait_recv()
    own_tok(other).wait_recv()

    def drained(slots):
        def drain(d, carry):
            for way in range(2):
                for slot in slots:
                    rs(way, slot, d).wait_send()
            return carry
        lax.fori_loop(0, n_d // PACK, drain, 0)

    own_meta(core).wait_send()
    own_tok(core).wait_send()
    for way in range(2):
        for hop in range(1, far + 1):
            if hop <= meta_hops[way]:
                ag_meta(way, hop, False)[0].wait_send()
                sib_meta(way, hop, core).wait_send()
            for kind in range(2):
                if hop <= far - kind:
                    for ck in range(AG_CHUNKS):
                        ag(way, kind, hop, ck, False)[0].wait_send()
                        sib_msg(way, kind, hop, ck, core).wait_send()
    drained(list(range(a_slot, a_slot + far - 1)) + list(range(b_slot, b_slot + far - 2)))
    phase(0, far, 2, lambda: None, last=True)
    drained([a_slot + far - 1, b_slot + far - 2])


def group_layer(n, tokens, ids, gates, slot_ids, w_gate, w_up, w_down, cap):
    rows, d_model = tokens.shape
    top_k = ids.shape[0]
    n_exp, _, d_ff = w_gate.shape
    far = n // 4
    spad = (cap + 63) // 64 * 64
    slots = n_exp * spad
    n_d = d_model // COLS
    loads = 2 * n_exp * d_ff // COLS + n_d * n_exp // 2
    n_w = next(k for k in (12, 8, 6, 4) if loads % k == 0 and k <= n_d * n_exp // 2)
    any_spec = pl.BlockSpec(memory_space=pl.ANY)
    dma = pltpu.SemaphoreType.DMA
    ag_shape = (2, 2, far, AG_CHUNKS)
    return pl.pallas_call(
        functools.partial(moe_kernel, (n, cap, spad, n_w)),
        out_shape=pltpu.VMEM((rows, d_model), BF16),
        in_specs=[any_spec] * 7,
        out_specs=pl.BlockSpec(memory_space=pltpu.VMEM),
        scratch_shapes=[
            pltpu.VMEM((n, rows, d_model), BF16),
            pltpu.VMEM((n, 2 * top_k, rows), F32),
            pltpu.VMEM((2, top_k, rows), jnp.int32),
            pltpu.VMEM((2, 2 * far + 1, n_d // PACK, PACK, rows // 2, COLS), F32),
            pltpu.VMEM((SIB_SLOTS, 2, rows, COLS), F32),
            pltpu.VMEM((2, 2, rows, COLS), F32),
            pltpu.VMEM((2, 2, rows, COLS), F32),
            pltpu.VMEM((n_w, d_model, COLS), BF16),
            pltpu.VMEM((n_exp, 4 * cap, d_model), BF16),
            pltpu.VMEM((n_exp, 4 * cap, d_ff), BF16),
            pltpu.VMEM((4, 3 * slots, COLS), BF16),
            pltpu.VMEM((4, rows, slots), BF16),
            pltpu.VMEM((4, slots, rows), BF16),
            pltpu.VMEM((n_exp, 4 * cap, 128), F32),
            dma((3 + 2 * AG_CHUNKS,)), dma((n_w, 2)),
            dma(ag_shape), dma(ag_shape), dma((2, far)), dma((2, far)),
            dma(ag_shape), dma(ag_shape), dma((2, far)), dma((2, far)),
            dma((2,)), dma((2,)),
            dma((2, 2 * far + 1, n_d // PACK)), dma((2, 2 * far + 1, n_d // PACK)),
            dma((2,)), dma((SIB_SLOTS,)),
            pltpu.SemaphoreType.REGULAR,
        ],
        compiler_params=pltpu.CompilerParams(collective_id=0, has_side_effects=True, vmem_limit_bytes=61 << 20),
    )(tokens, ids, gates, slot_ids, w_gate, w_up, w_down)


def solution(mesh):
    group_size = mesh.shape['ep']
    row_spec = P(('dp', 'ep'), None)
    expert_spec = P('ep', None, None)

    def per_device(tokens, expert_ids, gate_wts, slot_ids, w_gate, w_up, w_down):
        tok_dev, top_k = expert_ids.shape
        cap = CAP_NUM * tok_dev * top_k // (CAP_DEN * w_gate.shape[0] * group_size)
        return group_layer(group_size, tokens, expert_ids.T, gate_wts.T, slot_ids.T, w_gate, w_up, w_down, cap)

    return jax.shard_map(per_device, mesh=mesh, in_specs=(row_spec, row_spec, row_spec, row_spec, expert_spec, expert_spec, expert_spec), out_specs=row_spec, check_vma=False)
```

```python
import functools

import jax
import jax.numpy as jnp
from jax import lax
from jax.experimental import pallas as pl
from jax.experimental.pallas import tpu as pltpu
from jax.sharding import PartitionSpec as P

CAP_NUM = 3
CAP_DEN = 2
COLS = 256
AG_CHUNKS = 2
SIB_SLOTS = 4
PACK = 2
MESH = pl.DeviceIdType.MESH
BF16 = jnp.bfloat16
F32 = jnp.float32


def moe_kernel(cfg, tok_in, ids_in, gates_in, slots_in, wg, wu, wd, out,
               tok, meta, raw, ring, sib_in, sib_out, own, wbuf, xbuf, hbuf, obuf, ptbuf, pbuf, sgbuf,
               local_sem, w_sem, ag_s, ag_r, agm_s, agm_r, sb_s, sb_r, sbm_s, sbm_r, own_s, own_r,
               rs_s, rs_r, ss_s, ss_r, credit):
    n, cap, spad, n_w = cfg
    rows, d_model = tok_in.shape
    top_k = ids_in.shape[0]
    n_exp, _, d_ff = wg.shape
    chips = n // 2
    far = chips // 2
    half = rows // 2
    piece = half // AG_CHUNKS
    n_d = d_model // COLS
    n_f = d_ff // COLS
    slots = n_exp * spad
    up_loads = 2 * n_exp * n_f
    loads = up_loads + n_d * n_exp // 2
    total_chunks = (far + 1) * n_d
    a_slot, b_slot = 0, far + 1

    me = lax.axis_index('ep')
    chip, core = me // 2, me % 2
    other = 1 - core

    def place(chip_num, core_num):
        return ((chip_num + chips) % chips) * 2 + core_num

    sib = chip * 2 + other
    side = (place(chip + 1, core), place(chip - 1, core))
    sign = (1, -1)

    def load_up(idx, slot, start):
        step = idx // 2
        exp_num, col = step // n_f, pl.multiple_of((step % n_f) * COLS, COLS)
        start(pltpu.make_async_copy(wg.at[exp_num, :, pl.ds(col, COLS)], wbuf.at[slot], w_sem.at[slot, 0]))
        start(pltpu.make_async_copy(wu.at[exp_num, :, pl.ds(col, COLS)], wbuf.at[slot + 1], w_sem.at[slot + 1, 0]))

    def load_down(idx, slot, start):
        col, pair = pl.multiple_of((idx // (n_exp // 2)) * COLS, COLS), idx % (n_exp // 2)
        for k in range(2):
            start(pltpu.make_async_copy(wd.at[pair * 2 + k, :, pl.ds(col, COLS)], wbuf.at[slot, pl.ds(k * d_ff, d_ff)], w_sem.at[slot, k]))

    begin = lambda copy: copy.start()
    finish = lambda copy: copy.wait()

    def part_rows(way, kind, ck):
        upper = (way == 0) == (kind == 1)
        return pl.ds((half if upper else 0) + ck * piece, piece)

    def ag(way, kind, hop, ck, arriving):
        origin = place(chip - sign[way] * (hop if arriving else hop - 1), core)
        if isinstance(ck, int):
            view = tok.at[origin, part_rows(way, kind, ck)]
        else:
            base = half if (way == 0) == (kind == 1) else 0
            view = tok.at[origin, pl.ds(pl.multiple_of(base + ck * piece, piece), piece)]
        copy = pltpu.make_async_remote_copy(view, view, ag_s.at[way, kind, hop - 1, ck], ag_r.at[way, kind, hop - 1, ck], device_id={'ep': side[way]}, device_id_type=MESH)
        return copy, origin, view

    def ag_meta(way, hop, arriving):
        origin = place(chip - sign[way] * (hop if arriving else hop - 1), core)
        view = meta.at[origin]
        copy = pltpu.make_async_remote_copy(view, view, agm_s.at[way, hop - 1], agm_r.at[way, hop - 1], device_id={'ep': side[way]}, device_id_type=MESH)
        return copy, origin, view

    def to_sib(view, send_sem, recv_sem):
        return pltpu.make_async_remote_copy(view, view, send_sem, recv_sem, device_id={'ep': sib}, device_id_type=MESH)

    def sib_view(way, kind, hop, ck, core_num):
        origin = place(chip - sign[way] * hop, core_num)
        base = half if (way == 0) == (kind == 1) else 0
        return tok.at[origin, pl.ds(pl.multiple_of(base + ck * piece, piece), piece)]

    def sib_msg(way, kind, hop, ck, core_num):
        return to_sib(sib_view(way, kind, hop, ck, core_num), sb_s.at[way, kind, hop - 1, ck], sb_r.at[way, kind, hop - 1, ck])

    def sib_meta(way, hop, core_num):
        return to_sib(meta.at[place(chip - sign[way] * hop, core_num)], sbm_s.at[way, hop - 1], sbm_r.at[way, hop - 1])

    meta_hops = (far, far - 1)

    barrier = pltpu.get_barrier_semaphore()
    for dev in (side[0], side[1], sib):
        pl.semaphore_signal(barrier, inc=1, device_id={'ep': dev}, device_id_type=MESH)
    local = (pltpu.make_async_copy(ids_in, raw.at[0], local_sem.at[0]), pltpu.make_async_copy(slots_in, raw.at[1], local_sem.at[1]),
             pltpu.make_async_copy(gates_in, meta.at[me, pl.ds(top_k, top_k)], local_sem.at[2]))
    bands = [pltpu.make_async_copy(tok_in.at[part_rows(way, 0, ck)], tok.at[me, part_rows(way, 0, ck)], local_sem.at[3 + ck * 2 + way]) for ck in range(AG_CHUNKS) for way in range(2)]
    for copy in local + tuple(bands):
        copy.start()
    for copy in local[:2]:
        copy.wait()
    slot_ids = raw[1]
    meta[me, pl.ds(0, top_k), :] = jnp.where(slot_ids >= 0, raw[0] * cap + slot_ids - me * cap, -1).astype(F32)
    pl.semaphore_wait(barrier, 3)

    own_tok = lambda core_num: to_sib(tok.at[place(chip, core_num)], own_s.at[0], own_r.at[0])
    own_meta = lambda core_num: to_sib(meta.at[place(chip, core_num)], own_s.at[1], own_r.at[1])
    for ck in range(AG_CHUNKS):
        for way in range(2):
            bands[ck * 2 + way].wait()
            ag(way, 0, 1, ck, False)[0].start()
        if ck == 0:
            local[2].wait()
            for way in range(2):
                ag_meta(way, 1, False)[0].start()
    for idx in range(0, n_w, 2):
        load_up(jnp.int32(idx), idx, begin)
    obuf[...] = jnp.zeros_like(obuf)
    for hop in range(1, far + 1):
        for ck in range(AG_CHUNKS):
            for way in range(2):
                ag(way, 0, hop, ck, True)[0].wait_recv()
                if hop < far:
                    ag(way, 0, hop + 1, ck, False)[0].start()
                sib_msg(way, 0, hop, ck, core).start()
                if ck == 0 and hop <= meta_hops[way]:
                    ag_meta(way, hop, True)[0].wait_recv()
                    if hop < meta_hops[way]:
                        ag_meta(way, hop + 1, False)[0].start()
                    sib_meta(way, hop, core).start()
        if hop == far - 1:
            own_meta(core).start()
            own_tok(core).start()
            for ck in range(AG_CHUNKS):
                for way in range(2):
                    ag(way, 1, 1, ck, False)[0].start()

    def second_half_event(event):
        hop, ck = event // AG_CHUNKS + 1, event % AG_CHUNKS
        for way in range(2):
            ag(way, 1, hop, ck, True)[0].wait_recv()

            @pl.when(hop < far - 1)
            def _():
                ag(way, 1, hop + 1, ck, False)[0].start()
            sib_msg(way, 1, hop, ck, core).start()

    n_events = (far - 1) * AG_CHUNKS

    def rs(way, slot, d):
        return pltpu.make_async_remote_copy(ring.at[way, slot, d], ring.at[way, slot + 1, d], rs_s.at[way, slot, d], rs_r.at[way, slot + 1, d], device_id={'ep': side[way]}, device_id_type=MESH)

    def rs_wait(way, slot, d):
        @pl.when(d % PACK == 0)
        def _():
            rs_arrived(way, slot, d // PACK)

    def rs_send(way, slot, d):
        @pl.when(d % PACK == PACK - 1)
        def _():
            rs(way, slot, d // PACK).start()

    def rs_arrived(way, slot, d):
        pltpu.make_async_remote_copy(ring.at[way, slot, d], ring.at[way, slot, d], rs_s.at[way, slot, d], rs_r.at[way, slot, d], device_id={'ep': side[way]}, device_id_type=MESH).wait_recv()

    lane_rows = (pl.ds(0, half), pl.ds(half, half))

    def phase(dist, order, shards, arrive, last=False, events=False):
        width = shards // 2
        m_rows = shards * cap

        def shard_place(num):
            which = num % width
            step = dist if width == 1 else dist * (1 - 2 * which)
            return place(chip + step, jnp.where(num < width, core, other))

        def masks(num, carry):
            shard = shard_place(num)
            base = (me * n_exp * cap).astype(F32)
            row_num = lax.broadcasted_iota(jnp.int32, (slots, rows), 0)
            in_exp = row_num % spad
            want = jnp.where(in_exp < cap, (row_num // spad) * cap + in_exp, -7).astype(F32)
            codes = meta[shard, pl.ds(0, top_k), :] - base
            gates = meta[shard, pl.ds(top_k, top_k), :]
            hot = jnp.zeros((slots, rows), F32)
            gate = jnp.zeros((slots, rows), F32)
            for j in range(top_k):
                same = want == codes[j:j + 1, :]
                hot = jnp.where(same, 1.0, hot)
                gate = jnp.where(same, gates[j:j + 1, :], gate)
            slot_gate = jnp.broadcast_to(jnp.sum(gate, axis=1, keepdims=True), (slots, 128))
            first = pl.multiple_of(num * cap, 16)
            for e in range(n_exp):
                sgbuf[e, pl.ds(first, cap), :] = slot_gate[e * spad:e * spad + cap]
            ptbuf[num] = hot.T.astype(BF16)
            pbuf[num] = hot.astype(BF16)
            return carry

        def gather(num, carry):
            shard = shard_place(num)
            first = pl.multiple_of(num * cap, 16)
            pick = pbuf[num]
            for c in range(d_model // COLS):
                got = jnp.dot(pick, tok[shard, :, pl.ds(c * COLS, COLS)], preferred_element_type=F32).astype(BF16)
                for e in range(n_exp):
                    xbuf[e, pl.ds(first, cap), pl.ds(c * COLS, COLS)] = got[e * spad:e * spad + cap]
            return carry

        lax.fori_loop(0, shards, masks, 0)
        arrive()
        lax.fori_loop(0, shards, gather, 0)

        def up_step(step, carry):
            idx = step * 2
            slot = idx % n_w
            load_up(idx, slot, finish)
            e, col = step // n_f, pl.multiple_of((step % n_f) * COLS, COLS)
            x = xbuf[e, pl.ds(0, m_rows), :]
            a = jnp.dot(x, wbuf[slot], preferred_element_type=F32)
            u = jnp.dot(x, wbuf[slot + 1], preferred_element_type=F32)
            hbuf[e, pl.ds(0, m_rows), pl.ds(col, COLS)] = (jax.nn.silu(a) * u).astype(BF16)

            @pl.when(idx + n_w < up_loads)
            def _():
                load_up(idx + n_w, slot, begin)

            @pl.when(idx + n_w >= up_loads)
            def _():
                for k in range(2):
                    load_down(idx + n_w + k - up_loads, slot + k, begin)
            if events:
                every = max(n_exp * n_f // max(n_events - 2, 1), 1)

                @pl.when((step % every == every - 1) & (step // every < n_events - 2))
                def _():
                    second_half_event(step // every)
            return carry

        lax.fori_loop(0, n_exp * n_f, up_step, 0)

        def sib_share(d, waiting=False):
            count = order * n_d + d
            return pltpu.make_async_remote_copy(sib_out.at[d % 2, pl.ds(0, width)], sib_in.at[count % SIB_SLOTS, pl.ds(0, width)], ss_s.at[d % 2], ss_r.at[count % SIB_SLOTS], device_id={'ep': sib}, device_id_type=MESH)

        def close(d):
            count = order * n_d + d
            slot = count % SIB_SLOTS
            sib_share(d).wait_recv()
            mine = lambda i, r: own[d % 2, i, lane_rows[r], :] + sib_in[slot, i, lane_rows[r], :]
            if last:
                for way in range(2):
                    rs_wait(way, a_slot + far, d)
                    rs_wait(way, b_slot + far - 1, d)
                for r in range(2):
                    total = mine(0, r) + ring[r, a_slot + far, d // PACK, d % PACK] + ring[1 - r, b_slot + far - 1, d // PACK, d % PACK]
                    out[lane_rows[r], pl.ds(pl.multiple_of(d * COLS, COLS), COLS)] = total.astype(BF16)
            elif width == 1:
                for way in range(2):
                    ring[way, a_slot, d // PACK, d % PACK] = mine(0, way)
                    rs_send(way, a_slot, d)
            else:
                b_now = b_slot + far - 1 - dist
                a_now = a_slot + far - dist

                @pl.when(dist == far - 1)
                def _():
                    for way in range(2):
                        ring[way, b_slot, d // PACK, d % PACK] = mine(way, 1 - way)

                @pl.when(dist != far - 1)
                def _():
                    for way in range(2):
                        rs_wait(way, b_now, d)
                        ring[way, b_now, d // PACK, d % PACK] += mine(way, 1 - way)
                for way in range(2):
                    rs_send(way, b_now, d)
                for way in range(2):
                    rs_wait(way, a_now, d)
                    ring[way, a_now, d // PACK, d % PACK] += mine(way, way)
                    rs_send(way, a_now, d)

            @pl.when(count < total_chunks - SIB_SLOTS)
            def _():
                pl.semaphore_signal(credit, inc=1, device_id={'ep': sib}, device_id_type=MESH)

        def down_step(d, carry):
            for pair in range(n_exp // 2):
                idx = d * (n_exp // 2) + pair
                slot = (up_loads + idx) % n_w
                load_down(idx, slot, finish)
                for k in range(2):
                    e = pair * 2 + k
                    o = jnp.dot(hbuf[e, pl.ds(0, m_rows), :], wbuf[slot, pl.ds(k * d_ff, d_ff), :], preferred_element_type=F32)
                    g = sgbuf[e, pl.ds(0, m_rows), :]
                    o = o * jnp.concatenate([g] * (COLS // 128), axis=1)
                    for p in range(3):
                        cut = o.astype(BF16)
                        o = o - cut.astype(F32)
                        for i in range(shards):
                            obuf[i, pl.ds(p * slots + e * spad, cap), :] = cut[i * cap:(i + 1) * cap]

                @pl.when(up_loads + idx + n_w < loads)
                def _():
                    load_down(idx + n_w, slot, begin)
                if not last:
                    @pl.when((up_loads + idx + n_w >= loads) & ((up_loads + idx + n_w - loads) % 2 == 1))
                    def _():
                        load_up(up_loads + idx + n_w - loads - 1, slot - 1, begin)

            @pl.when(d >= 2)
            def _():
                sib_share(d).wait_send()

            @pl.when(order * n_d + d >= SIB_SLOTS)
            def _():
                pl.semaphore_wait(credit, 1)
            for i in list(range(width, shards)) + list(range(width)):
                pt = ptbuf[i]
                share = jnp.dot(pt, obuf[i, pl.ds(0, slots), :], preferred_element_type=F32)
                for p in range(1, 3):
                    share += jnp.dot(pt, obuf[i, pl.ds(p * slots, slots), :], preferred_element_type=F32)
                if i >= width:
                    sib_out[d % 2, i - width] = share
                else:
                    own[d % 2, i] = share
                if i == shards - 1:
                    sib_share(d).start()

            @pl.when(d >= 1)
            def _():
                close(d - 1)
            if events:
                @pl.when(d == n_d // 2 - 1)
                def _():
                    second_half_event(n_events - 2)
            return carry

        lax.fori_loop(0, n_d, down_step, 0)
        close(jnp.int32(n_d - 1))
        for d in range(n_d - 2, n_d):
            sib_share(d).wait_send()

    def far_rows():
        for way in range(2):
            for ck in range(AG_CHUNKS):
                sib_msg(way, 0, far, ck, other).wait_recv()

    for way in range(2):
        if far <= meta_hops[way]:
            sib_meta(way, far, other).wait_recv()
    phase(far, 0, 2, far_rows, events=True)

    def middle(order, carry):
        dist = far - order

        def rows_of():
            @pl.when(order == 1)
            def _():
                second_half_event(n_events - 1)
            for way in range(2):
                for kind in range(2):
                    for ck in range(AG_CHUNKS):
                        sib_msg(way, kind, dist, ck, other).wait_recv()

        for way in range(2):
            sib_meta(way, dist, other).wait_recv()
        phase(dist, order, 4, rows_of)
        return carry

    lax.fori_loop(1, far, middle, 0)
    own_meta(other).wait_recv()
    own_tok(other).wait_recv()

    def drained(slots):
        def drain(d, carry):
            for way in range(2):
                for slot in slots:
                    rs(way, slot, d).wait_send()
            return carry
        lax.fori_loop(0, n_d // PACK, drain, 0)

    own_meta(core).wait_send()
    own_tok(core).wait_send()
    for way in range(2):
        for hop in range(1, far + 1):
            if hop <= meta_hops[way]:
                ag_meta(way, hop, False)[0].wait_send()
                sib_meta(way, hop, core).wait_send()
            for kind in range(2):
                if hop <= far - kind:
                    for ck in range(AG_CHUNKS):
                        ag(way, kind, hop, ck, False)[0].wait_send()
                        sib_msg(way, kind, hop, ck, core).wait_send()
    drained(list(range(a_slot, a_slot + far - 1)) + list(range(b_slot, b_slot + far - 2)))
    phase(0, far, 2, lambda: None, last=True)
    drained([a_slot + far - 1, b_slot + far - 2])


def group_layer(n, tokens, ids, gates, slot_ids, w_gate, w_up, w_down, cap):
    rows, d_model = tokens.shape
    top_k = ids.shape[0]
    n_exp, _, d_ff = w_gate.shape
    far = n // 4
    spad = (cap + 63) // 64 * 64
    slots = n_exp * spad
    n_d = d_model // COLS
    loads = 2 * n_exp * d_ff // COLS + n_d * n_exp // 2
    n_w = next(k for k in (8, 6, 4) if loads % k == 0 and k <= n_d * n_exp // 2)
    any_spec = pl.BlockSpec(memory_space=pl.ANY)
    dma = pltpu.SemaphoreType.DMA
    ag_shape = (2, 2, far, AG_CHUNKS)
    return pl.pallas_call(
        functools.partial(moe_kernel, (n, cap, spad, n_w)),
        out_shape=pltpu.VMEM((rows, d_model), BF16),
        in_specs=[any_spec] * 7,
        out_specs=pl.BlockSpec(memory_space=pltpu.VMEM),
        scratch_shapes=[
            pltpu.VMEM((n, rows, d_model), BF16),
            pltpu.VMEM((n, 2 * top_k, rows), F32),
            pltpu.VMEM((2, top_k, rows), jnp.int32),
            pltpu.VMEM((2, 2 * far + 1, n_d // PACK, PACK, rows // 2, COLS), F32),
            pltpu.VMEM((SIB_SLOTS, 2, rows, COLS), F32),
            pltpu.VMEM((2, 2, rows, COLS), F32),
            pltpu.VMEM((2, 2, rows, COLS), F32),
            pltpu.VMEM((n_w, d_model, COLS), BF16),
            pltpu.VMEM((n_exp, 4 * cap, d_model), BF16),
            pltpu.VMEM((n_exp, 4 * cap, d_ff), BF16),
            pltpu.VMEM((4, 3 * slots, COLS), BF16),
            pltpu.VMEM((4, rows, slots), BF16),
            pltpu.VMEM((4, slots, rows), BF16),
            pltpu.VMEM((n_exp, 4 * cap, 128), F32),
            dma((3 + 2 * AG_CHUNKS,)), dma((n_w, 2)),
            dma(ag_shape), dma(ag_shape), dma((2, far)), dma((2, far)),
            dma(ag_shape), dma(ag_shape), dma((2, far)), dma((2, far)),
            dma((2,)), dma((2,)),
            dma((2, 2 * far + 1, n_d // PACK)), dma((2, 2 * far + 1, n_d // PACK)),
            dma((2,)), dma((SIB_SLOTS,)),
            pltpu.SemaphoreType.REGULAR,
        ],
        compiler_params=pltpu.CompilerParams(collective_id=0, has_side_effects=True, vmem_limit_bytes=58 << 20),
    )(tokens, ids, gates, slot_ids, w_gate, w_up, w_down)


def solution(mesh):
    group_size = mesh.shape['ep']
    row_spec = P(('dp', 'ep'), None)
    expert_spec = P('ep', None, None)

    def per_device(tokens, expert_ids, gate_wts, slot_ids, w_gate, w_up, w_down):
        tok_dev, top_k = expert_ids.shape
        cap = CAP_NUM * tok_dev * top_k // (CAP_DEN * w_gate.shape[0] * group_size)
        return group_layer(group_size, tokens, expert_ids.T, gate_wts.T, slot_ids.T, w_gate, w_up, w_down, cap)

    return jax.shard_map(per_device, mesh=mesh, in_specs=(row_spec, row_spec, row_spec, row_spec, expert_spec, expert_spec, expert_spec), out_specs=row_spec, check_vma=False)
```

```python
import functools

import jax
import jax.numpy as jnp
from jax import lax
from jax.experimental import pallas as pl
from jax.experimental.pallas import tpu as pltpu
from jax.sharding import PartitionSpec as P

CAP_NUM = 3
CAP_DEN = 2
COLS = 256
AG_CHUNKS = 2
SIB_SLOTS = 4
PACK = 2
MESH = pl.DeviceIdType.MESH
BF16 = jnp.bfloat16
F32 = jnp.float32


def moe_kernel(cfg, tok_in, ids_in, gates_in, slots_in, wg, wu, wd, out,
               tok, meta, raw, ring, sib_in, sib_out, own, wbuf, xbuf, hbuf, obuf, ptbuf, sgbuf,
               local_sem, w_sem, ag_s, ag_r, agm_s, agm_r, sb_s, sb_r, sbm_s, sbm_r, own_s, own_r, guest_s, guest_r,
               rs_s, rs_r, ss_s, ss_r, credit):
    n, cap, spad, n_w = cfg
    rows, d_model = tok_in.shape
    top_k = ids_in.shape[0]
    n_exp, _, d_ff = wg.shape
    chips = n // 2
    far = chips // 2
    half = rows // 2
    piece = half // AG_CHUNKS
    n_d = d_model // COLS
    n_f = d_ff // COLS
    slots = n_exp * spad
    up_loads = 2 * n_exp * n_f
    loads = up_loads + n_d * n_exp // 2
    total_chunks = (far + 1) * n_d
    a_slot, b_slot = 0, far + 1

    me = lax.axis_index('ep')
    chip, core = me // 2, me % 2
    other = 1 - core

    def place(chip_num, core_num):
        return ((chip_num + chips) % chips) * 2 + core_num

    sib = chip * 2 + other
    side = (place(chip + 1, core), place(chip - 1, core))
    sign = (1, -1)

    def load_up(idx, slot, start):
        step = idx // 2
        exp_num, col = step // n_f, pl.multiple_of((step % n_f) * COLS, COLS)
        start(pltpu.make_async_copy(wg.at[exp_num, :, pl.ds(col, COLS)], wbuf.at[slot], w_sem.at[slot, 0]))
        start(pltpu.make_async_copy(wu.at[exp_num, :, pl.ds(col, COLS)], wbuf.at[slot + 1], w_sem.at[slot + 1, 0]))

    def load_down(idx, slot, start):
        col, pair = pl.multiple_of((idx // (n_exp // 2)) * COLS, COLS), idx % (n_exp // 2)
        for k in range(2):
            start(pltpu.make_async_copy(wd.at[pair * 2 + k, :, pl.ds(col, COLS)], wbuf.at[slot, pl.ds(k * d_ff, d_ff)], w_sem.at[slot, k]))

    begin = lambda copy: copy.start()
    finish = lambda copy: copy.wait()

    def part_rows(way, kind, ck):
        upper = (way == 0) == (kind == 1)
        return pl.ds((half if upper else 0) + ck * piece, piece)

    def ag(way, kind, hop, ck, arriving):
        origin = place(chip - sign[way] * (hop if arriving else hop - 1), core)
        if isinstance(ck, int):
            view = tok.at[origin, part_rows(way, kind, ck)]
        else:
            base = half if (way == 0) == (kind == 1) else 0
            view = tok.at[origin, pl.ds(pl.multiple_of(base + ck * piece, piece), piece)]
        copy = pltpu.make_async_remote_copy(view, view, ag_s.at[way, kind, hop - 1, ck], ag_r.at[way, kind, hop - 1, ck], device_id={'ep': side[way]}, device_id_type=MESH)
        return copy, origin, view

    def ag_meta(way, hop, arriving):
        origin = place(chip - sign[way] * (hop if arriving else hop - 1), core)
        view = meta.at[origin]
        copy = pltpu.make_async_remote_copy(view, view, agm_s.at[way, hop - 1], agm_r.at[way, hop - 1], device_id={'ep': side[way]}, device_id_type=MESH)
        return copy, origin, view

    def to_sib(view, send_sem, recv_sem):
        return pltpu.make_async_remote_copy(view, view, send_sem, recv_sem, device_id={'ep': sib}, device_id_type=MESH)

    def sib_view(way, kind, hop, ck, core_num):
        origin = place(chip - sign[way] * hop, core_num)
        base = half if (way == 0) == (kind == 1) else 0
        return tok.at[origin, pl.ds(pl.multiple_of(base + ck * piece, piece), piece)]

    def sib_msg(way, kind, hop, ck, core_num):
        return to_sib(sib_view(way, kind, hop, ck, core_num), sb_s.at[way, kind, hop - 1, ck], sb_r.at[way, kind, hop - 1, ck])

    def sib_meta(way, hop, core_num):
        return to_sib(meta.at[place(chip - sign[way] * hop, core_num)], sbm_s.at[way, hop - 1], sbm_r.at[way, hop - 1])

    meta_hops = (far, far - 1)
    swap_ck = AG_CHUNKS - 1

    def split_rows(way, num):
        return pl.ds((0 if way == 0 else half) + swap_ck * piece + num * (piece // 2), piece // 2)

    def stay(way, arriving):
        origin = place(chip - sign[way] * (far if arriving else far - 1), 1)
        view = tok.at[origin, split_rows(way, 0)]
        return pltpu.make_async_remote_copy(view, view, ag_s.at[way, 0, far - 1, swap_ck], ag_r.at[way, 0, far - 1, swap_ck], device_id={'ep': side[way]}, device_id_type=MESH)

    def stay_sib(way):
        origin = place(chip - sign[way] * far, 1)
        return to_sib(tok.at[origin, split_rows(way, 0)], sb_s.at[way, 0, far - 1, swap_ck], sb_r.at[way, 0, far - 1, swap_ck])

    def guest(way, arriving):
        origin = place(chip - sign[way] * (far if arriving else far - 1), 1)
        view = tok.at[origin, split_rows(way, 1)]
        return pltpu.make_async_remote_copy(view, view, guest_s.at[way, 0], guest_r.at[way, 0], device_id={'ep': side[way]}, device_id_type=MESH)

    def guest_sib(way):
        origin = place(chip - sign[way] * far, 1)
        return to_sib(tok.at[origin, split_rows(way, 1)], guest_s.at[way, 1], guest_r.at[way, 1])

    barrier = pltpu.get_barrier_semaphore()
    for dev in (side[0], side[1], sib):
        pl.semaphore_signal(barrier, inc=1, device_id={'ep': dev}, device_id_type=MESH)
    local = (pltpu.make_async_copy(ids_in, raw.at[0], local_sem.at[0]), pltpu.make_async_copy(slots_in, raw.at[1], local_sem.at[1]),
             pltpu.make_async_copy(gates_in, meta.at[me, pl.ds(top_k, top_k)], local_sem.at[2]))
    bands = [pltpu.make_async_copy(tok_in.at[part_rows(way, 0, ck)], tok.at[me, part_rows(way, 0, ck)], local_sem.at[3 + ck * 2 + way]) for ck in range(AG_CHUNKS) for way in range(2)]
    for copy in local + tuple(bands):
        copy.start()
    pl.semaphore_wait(barrier, 3)

    own_tok = lambda core_num: to_sib(tok.at[place(chip, core_num)], own_s.at[0], own_r.at[0])
    own_meta = lambda core_num: to_sib(meta.at[place(chip, core_num)], own_s.at[1], own_r.at[1])
    for ck in range(AG_CHUNKS):
        for way in range(2):
            bands[ck * 2 + way].wait()
            ag(way, 0, 1, ck, False)[0].start()
        if ck == 0:
            for copy in local:
                copy.wait()
            slot_ids = raw[1]
            meta[me, pl.ds(0, top_k), :] = jnp.where(slot_ids >= 0, raw[0] * cap + slot_ids - me * cap, -1).astype(F32)
    for way in range(2):
        ag_meta(way, 1, False)[0].start()
    own_meta(core).start()
    own_tok(core).start()
    for idx in range(0, n_w, 2):
        load_up(jnp.int32(idx), idx, begin)
    obuf[...] = jnp.zeros_like(obuf)
    for hop in range(1, far + 1):
        for ck in range(AG_CHUNKS):
            for way in range(2):
                if hop == far and ck == swap_ck:
                    @pl.when(core == 0)
                    def _():
                        ag(way, 0, hop, ck, True)[0].wait_recv()
                        sib_msg(way, 0, hop, ck, core).start()
                        guest(way, True).wait_recv()
                        guest_sib(way).start()

                    @pl.when(core == 1)
                    def _():
                        stay(way, True).wait_recv()
                        stay_sib(way).start()
                    continue
                ag(way, 0, hop, ck, True)[0].wait_recv()
                if hop + 1 == far and ck == swap_ck:
                    sib_msg(way, 0, hop, ck, core).start()

                    @pl.when(core == 0)
                    def _():
                        ag(way, 0, hop + 1, ck, False)[0].start()
                        sib_msg(way, 0, hop, ck, other).wait_recv()
                        guest(way, False).start()

                    @pl.when(core == 1)
                    def _():
                        stay(way, False).start()
                    continue
                if hop < far:
                    ag(way, 0, hop + 1, ck, False)[0].start()
                sib_msg(way, 0, hop, ck, core).start()
        for way in range(2):
            if hop <= meta_hops[way]:
                ag_meta(way, hop, True)[0].wait_recv()
                if hop < meta_hops[way]:
                    ag_meta(way, hop + 1, False)[0].start()
                sib_meta(way, hop, core).start()
        if hop == far - 1:
            for ck in range(AG_CHUNKS):
                for way in range(2):
                    ag(way, 1, 1, ck, False)[0].start()

    def second_half_event(event):
        hop, ck = event // AG_CHUNKS + 1, event % AG_CHUNKS
        for way in range(2):
            ag(way, 1, hop, ck, True)[0].wait_recv()

            @pl.when(hop < far - 1)
            def _():
                ag(way, 1, hop + 1, ck, False)[0].start()
            sib_msg(way, 1, hop, ck, core).start()

    n_events = (far - 1) * AG_CHUNKS

    def rs(way, slot, d):
        return pltpu.make_async_remote_copy(ring.at[way, slot, d], ring.at[way, slot + 1, d], rs_s.at[way, slot, d], rs_r.at[way, slot + 1, d], device_id={'ep': side[way]}, device_id_type=MESH)

    def rs_wait(way, slot, d):
        @pl.when(d % PACK == 0)
        def _():
            rs_arrived(way, slot, d // PACK)

    def rs_send(way, slot, d):
        @pl.when(d % PACK == PACK - 1)
        def _():
            rs(way, slot, d // PACK).start()

    def rs_arrived(way, slot, d):
        pltpu.make_async_remote_copy(ring.at[way, slot, d], ring.at[way, slot, d], rs_s.at[way, slot, d], rs_r.at[way, slot, d], device_id={'ep': side[way]}, device_id_type=MESH).wait_recv()

    lane_rows = (pl.ds(0, half), pl.ds(half, half))

    def phase(dist, order, shards, last=False, events=False):
        width = shards // 2
        m_rows = shards * cap

        def shard_place(num):
            which = num % width
            step = dist if width == 1 else dist * (1 - 2 * which)
            return place(chip + step, jnp.where(num < width, core, other))

        def gather(num, carry):
            shard = shard_place(num)
            base = (me * n_exp * cap).astype(F32)
            row_num = lax.broadcasted_iota(jnp.int32, (slots, rows), 0)
            in_exp = row_num % spad
            want = jnp.where(in_exp < cap, (row_num // spad) * cap + in_exp, -7).astype(F32)
            codes = meta[shard, pl.ds(0, top_k), :] - base
            gates = meta[shard, pl.ds(top_k, top_k), :]
            hot = jnp.zeros((slots, rows), F32)
            gate = jnp.zeros((slots, rows), F32)
            for j in range(top_k):
                same = want == codes[j:j + 1, :]
                hot = jnp.where(same, 1.0, hot)
                gate = jnp.where(same, gates[j:j + 1, :], gate)
            slot_gate = jnp.broadcast_to(jnp.sum(gate, axis=1, keepdims=True), (slots, 128))
            first = pl.multiple_of(num * cap, 16)
            for e in range(n_exp):
                sgbuf[e, pl.ds(first, cap), :] = slot_gate[e * spad:e * spad + cap]
            ptbuf[num] = hot.T.astype(BF16)
            pick = hot.astype(BF16)
            for c in range(d_model // COLS):
                got = jnp.dot(pick, tok[shard, :, pl.ds(c * COLS, COLS)], preferred_element_type=F32).astype(BF16)
                for e in range(n_exp):
                    xbuf[e, pl.ds(first, cap), pl.ds(c * COLS, COLS)] = got[e * spad:e * spad + cap]
            return carry

        lax.fori_loop(0, shards, gather, 0)

        def up_step(step, carry):
            idx = step * 2
            slot = idx % n_w
            load_up(idx, slot, finish)
            e, col = step // n_f, pl.multiple_of((step % n_f) * COLS, COLS)
            x = xbuf[e, pl.ds(0, m_rows), :]
            a = jnp.dot(x, wbuf[slot], preferred_element_type=F32)
            u = jnp.dot(x, wbuf[slot + 1], preferred_element_type=F32)
            hbuf[e, pl.ds(0, m_rows), pl.ds(col, COLS)] = (jax.nn.silu(a) * u).astype(BF16)

            @pl.when(idx + n_w < up_loads)
            def _():
                load_up(idx + n_w, slot, begin)

            @pl.when(idx + n_w >= up_loads)
            def _():
                for k in range(2):
                    load_down(idx + n_w + k - up_loads, slot + k, begin)
            if events:
                every = max(n_exp * n_f // max(n_events - 2, 1), 1)

                @pl.when((step % every == every - 1) & (step // every < n_events - 2))
                def _():
                    second_half_event(step // every)
            return carry

        lax.fori_loop(0, n_exp * n_f, up_step, 0)

        def sib_share(d, waiting=False):
            count = order * n_d + d
            return pltpu.make_async_remote_copy(sib_out.at[d % 2, pl.ds(0, width)], sib_in.at[count % SIB_SLOTS, pl.ds(0, width)], ss_s.at[d % 2], ss_r.at[count % SIB_SLOTS], device_id={'ep': sib}, device_id_type=MESH)

        def close(d):
            count = order * n_d + d
            slot = count % SIB_SLOTS
            sib_share(d).wait_recv()
            mine = lambda i, r: own[d % 2, i, lane_rows[r], :] + sib_in[slot, i, lane_rows[r], :]
            if last:
                for way in range(2):
                    rs_wait(way, a_slot + far, d)
                    rs_wait(way, b_slot + far - 1, d)
                for r in range(2):
                    total = mine(0, r) + ring[r, a_slot + far, d // PACK, d % PACK] + ring[1 - r, b_slot + far - 1, d // PACK, d % PACK]
                    out[lane_rows[r], pl.ds(pl.multiple_of(d * COLS, COLS), COLS)] = total.astype(BF16)
            elif width == 1:
                for way in range(2):
                    ring[way, a_slot, d // PACK, d % PACK] = mine(0, way)
                    rs_send(way, a_slot, d)
            else:
                b_now = b_slot + far - 1 - dist
                a_now = a_slot + far - dist

                @pl.when(dist == far - 1)
                def _():
                    for way in range(2):
                        ring[way, b_slot, d // PACK, d % PACK] = mine(way, 1 - way)

                @pl.when(dist != far - 1)
                def _():
                    for way in range(2):
                        rs_wait(way, b_now, d)
                        ring[way, b_now, d // PACK, d % PACK] += mine(way, 1 - way)
                for way in range(2):
                    rs_send(way, b_now, d)
                for way in range(2):
                    rs_wait(way, a_now, d)
                    ring[way, a_now, d // PACK, d % PACK] += mine(way, way)
                    rs_send(way, a_now, d)

            @pl.when(count < total_chunks - SIB_SLOTS)
            def _():
                pl.semaphore_signal(credit, inc=1, device_id={'ep': sib}, device_id_type=MESH)

        def down_step(d, carry):
            for pair in range(n_exp // 2):
                idx = d * (n_exp // 2) + pair
                slot = (up_loads + idx) % n_w
                load_down(idx, slot, finish)
                for k in range(2):
                    e = pair * 2 + k
                    o = jnp.dot(hbuf[e, pl.ds(0, m_rows), :], wbuf[slot, pl.ds(k * d_ff, d_ff), :], preferred_element_type=F32)
                    g = sgbuf[e, pl.ds(0, m_rows), :]
                    o = o * jnp.concatenate([g] * (COLS // 128), axis=1)
                    for p in range(3):
                        cut = o.astype(BF16)
                        o = o - cut.astype(F32)
                        for i in range(shards):
                            obuf[i, pl.ds(p * slots + e * spad, cap), :] = cut[i * cap:(i + 1) * cap]

                @pl.when(up_loads + idx + n_w < loads)
                def _():
                    load_down(idx + n_w, slot, begin)
                if not last:
                    @pl.when((up_loads + idx + n_w >= loads) & ((up_loads + idx + n_w - loads) % 2 == 1))
                    def _():
                        load_up(up_loads + idx + n_w - loads - 1, slot - 1, begin)

            @pl.when(d >= 2)
            def _():
                sib_share(d).wait_send()

            @pl.when(order * n_d + d >= SIB_SLOTS)
            def _():
                pl.semaphore_wait(credit, 1)
            for i in list(range(width, shards)) + list(range(width)):
                pt = ptbuf[i]
                share = jnp.dot(pt, obuf[i, pl.ds(0, slots), :], preferred_element_type=F32)
                for p in range(1, 3):
                    share += jnp.dot(pt, obuf[i, pl.ds(p * slots, slots), :], preferred_element_type=F32)
                if i >= width:
                    sib_out[d % 2, i - width] = share
                else:
                    own[d % 2, i] = share
                if i == shards - 1:
                    sib_share(d).start()

            @pl.when(d >= 1)
            def _():
                close(d - 1)
            if events:
                for k in range(2):
                    @pl.when(d == (k + 1) * n_d // 2 - 1)
                    def _():
                        second_half_event(n_events - 2 + k)
            return carry

        lax.fori_loop(0, n_d, down_step, 0)
        close(jnp.int32(n_d - 1))
        for d in range(n_d - 2, n_d):
            sib_share(d).wait_send()

    for way in range(2):
        if far <= meta_hops[way]:
            sib_meta(way, far, other).wait_recv()
        for ck in range(AG_CHUNKS):
            if ck != swap_ck:
                sib_msg(way, 0, far, ck, other).wait_recv()

        @pl.when(core == 0)
        def _():
            stay_sib(way).wait_recv()

        @pl.when(core == 1)
        def _():
            sib_msg(way, 0, far, swap_ck, other).wait_recv()
            guest_sib(way).wait_recv()
    phase(far, 0, 2, events=True)

    def middle(order, carry):
        dist = far - order
        for way in range(2):
            sib_meta(way, dist, other).wait_recv()
            for kind in range(2):
                for ck in range(AG_CHUNKS):
                    if kind == 0 and ck == swap_ck:
                        @pl.when((core == 1) | (dist != far - 1))
                        def _():
                            sib_msg(way, kind, dist, ck, other).wait_recv()
                    else:
                        sib_msg(way, kind, dist, ck, other).wait_recv()
        phase(dist, order, 4)
        return carry

    lax.fori_loop(1, far, middle, 0)
    own_meta(other).wait_recv()
    own_tok(other).wait_recv()
    phase(0, far, 2, last=True)

    own_meta(core).wait_send()
    own_tok(core).wait_send()
    for way in range(2):
        for hop in range(1, far + 1):
            if hop <= meta_hops[way]:
                ag_meta(way, hop, False)[0].wait_send()
                sib_meta(way, hop, core).wait_send()
            for kind in range(2):
                if hop <= far - kind:
                    for ck in range(AG_CHUNKS):
                        if kind == 0 and hop == far and ck == swap_ck:
                            @pl.when(core == 0)
                            def _():
                                ag(way, kind, hop, ck, False)[0].wait_send()
                                sib_msg(way, kind, hop, ck, core).wait_send()
                                guest(way, False).wait_send()
                                guest_sib(way).wait_send()

                            @pl.when(core == 1)
                            def _():
                                stay(way, False).wait_send()
                                stay_sib(way).wait_send()
                        else:
                            ag(way, kind, hop, ck, False)[0].wait_send()
                            sib_msg(way, kind, hop, ck, core).wait_send()

        def drain(d, carry):
            for slot in list(range(a_slot, a_slot + far)) + list(range(b_slot, b_slot + far - 1)):
                rs(way, slot, d).wait_send()
            return carry
        lax.fori_loop(0, n_d // PACK, drain, 0)


def group_layer(n, tokens, ids, gates, slot_ids, w_gate, w_up, w_down, cap):
    rows, d_model = tokens.shape
    top_k = ids.shape[0]
    n_exp, _, d_ff = w_gate.shape
    far = n // 4
    spad = (cap + 63) // 64 * 64
    slots = n_exp * spad
    n_d = d_model // COLS
    loads = 2 * n_exp * d_ff // COLS + n_d * n_exp // 2
    n_w = 8 if loads % 8 == 0 else 4
    any_spec = pl.BlockSpec(memory_space=pl.ANY)
    dma = pltpu.SemaphoreType.DMA
    ag_shape = (2, 2, far, AG_CHUNKS)
    return pl.pallas_call(
        functools.partial(moe_kernel, (n, cap, spad, n_w)),
        out_shape=pltpu.VMEM((rows, d_model), BF16),
        in_specs=[any_spec] * 7,
        out_specs=pl.BlockSpec(memory_space=pltpu.VMEM),
        scratch_shapes=[
            pltpu.VMEM((n, rows, d_model), BF16),
            pltpu.VMEM((n, 2 * top_k, rows), F32),
            pltpu.VMEM((2, top_k, rows), jnp.int32),
            pltpu.VMEM((2, 2 * far + 1, n_d // PACK, PACK, rows // 2, COLS), F32),
            pltpu.VMEM((SIB_SLOTS, 2, rows, COLS), F32),
            pltpu.VMEM((2, 2, rows, COLS), F32),
            pltpu.VMEM((2, 2, rows, COLS), F32),
            pltpu.VMEM((n_w, d_model, COLS), BF16),
            pltpu.VMEM((n_exp, 4 * cap, d_model), BF16),
            pltpu.VMEM((n_exp, 4 * cap, d_ff), BF16),
            pltpu.VMEM((4, 3 * slots, COLS), BF16),
            pltpu.VMEM((4, rows, slots), BF16),
            pltpu.VMEM((n_exp, 4 * cap, 128), F32),
            dma((3 + 2 * AG_CHUNKS,)), dma((n_w, 2)),
            dma(ag_shape), dma(ag_shape), dma((2, far)), dma((2, far)),
            dma(ag_shape), dma(ag_shape), dma((2, far)), dma((2, far)),
            dma((2,)), dma((2,)), dma((2, 2)), dma((2, 2)),
            dma((2, 2 * far + 1, n_d // PACK)), dma((2, 2 * far + 1, n_d // PACK)),
            dma((2,)), dma((SIB_SLOTS,)),
            pltpu.SemaphoreType.REGULAR,
        ],
        compiler_params=pltpu.CompilerParams(collective_id=0, has_side_effects=True, vmem_limit_bytes=58 << 20),
    )(tokens, ids, gates, slot_ids, w_gate, w_up, w_down)


def solution(mesh):
    group_size = mesh.shape['ep']
    row_spec = P(('dp', 'ep'), None)
    expert_spec = P('ep', None, None)

    def per_device(tokens, expert_ids, gate_wts, slot_ids, w_gate, w_up, w_down):
        tok_dev, top_k = expert_ids.shape
        cap = CAP_NUM * tok_dev * top_k // (CAP_DEN * w_gate.shape[0] * group_size)
        return group_layer(group_size, tokens, expert_ids.T, gate_wts.T, slot_ids.T, w_gate, w_up, w_down, cap)

    return jax.shard_map(per_device, mesh=mesh, in_specs=(row_spec, row_spec, row_spec, row_spec, expert_spec, expert_spec, expert_spec), out_specs=row_spec, check_vma=False)
```

```python
import functools

import jax
import jax.numpy as jnp
from jax import lax
from jax.experimental import pallas as pl
from jax.experimental.pallas import tpu as pltpu
from jax.sharding import PartitionSpec as P

CAP_NUM = 3
CAP_DEN = 2
COLS = 256
AG_CHUNKS = 2
SIB_SLOTS = 4
PACK = 2
MESH = pl.DeviceIdType.MESH
BF16 = jnp.bfloat16
F32 = jnp.float32


def moe_kernel(cfg, tok_in, ids_in, gates_in, slots_in, wg, wu, wd, out,
               tok, meta, raw, ring, sib_in, sib_out, own, wbuf, xbuf, hbuf, obuf, ptbuf, sgbuf,
               local_sem, w_sem, ag_s, ag_r, agm_s, agm_r, sb_s, sb_r, sbm_s, sbm_r, own_s, own_r,
               rs_s, rs_r, ss_s, ss_r, credit):
    n, cap, spad, n_w = cfg
    rows, d_model = tok_in.shape
    top_k = ids_in.shape[0]
    n_exp, _, d_ff = wg.shape
    chips = n // 2
    far = chips // 2
    half = rows // 2
    piece = half // AG_CHUNKS
    n_d = d_model // COLS
    n_f = d_ff // COLS
    slots = n_exp * spad
    up_loads = 2 * n_exp * n_f
    loads = up_loads + n_d * n_exp // 2
    total_chunks = (far + 1) * n_d
    a_slot, b_slot = 0, far + 1

    me = lax.axis_index('ep')
    chip, core = me // 2, me % 2
    other = 1 - core

    def place(chip_num, core_num):
        return ((chip_num + chips) % chips) * 2 + core_num

    sib = chip * 2 + other
    side = (place(chip + 1, core), place(chip - 1, core))
    sign = (1, -1)

    def load_up(idx, slot, start):
        step = idx // 2
        exp_num, col = step // n_f, pl.multiple_of((step % n_f) * COLS, COLS)
        start(pltpu.make_async_copy(wg.at[exp_num, :, pl.ds(col, COLS)], wbuf.at[slot], w_sem.at[slot, 0]))
        start(pltpu.make_async_copy(wu.at[exp_num, :, pl.ds(col, COLS)], wbuf.at[slot + 1], w_sem.at[slot + 1, 0]))

    def load_down(idx, slot, start):
        col, pair = pl.multiple_of((idx // (n_exp // 2)) * COLS, COLS), idx % (n_exp // 2)
        for k in range(2):
            start(pltpu.make_async_copy(wd.at[pair * 2 + k, :, pl.ds(col, COLS)], wbuf.at[slot, pl.ds(k * d_ff, d_ff)], w_sem.at[slot, k]))

    begin = lambda copy: copy.start()
    finish = lambda copy: copy.wait()

    def part_rows(way, kind, ck):
        upper = (way == 0) == (kind == 1)
        return pl.ds((half if upper else 0) + ck * piece, piece)

    def ag(way, kind, hop, ck, arriving):
        origin = place(chip - sign[way] * (hop if arriving else hop - 1), core)
        if isinstance(ck, int):
            view = tok.at[origin, part_rows(way, kind, ck)]
        else:
            base = half if (way == 0) == (kind == 1) else 0
            view = tok.at[origin, pl.ds(pl.multiple_of(base + ck * piece, piece), piece)]
        copy = pltpu.make_async_remote_copy(view, view, ag_s.at[way, kind, hop - 1, ck], ag_r.at[way, kind, hop - 1, ck], device_id={'ep': side[way]}, device_id_type=MESH)
        return copy, origin, view

    def ag_meta(way, hop, arriving):
        origin = place(chip - sign[way] * (hop if arriving else hop - 1), core)
        view = meta.at[origin]
        copy = pltpu.make_async_remote_copy(view, view, agm_s.at[way, hop - 1], agm_r.at[way, hop - 1], device_id={'ep': side[way]}, device_id_type=MESH)
        return copy, origin, view

    def to_sib(view, send_sem, recv_sem):
        return pltpu.make_async_remote_copy(view, view, send_sem, recv_sem, device_id={'ep': sib}, device_id_type=MESH)

    def sib_view(way, kind, hop, ck, core_num):
        origin = place(chip - sign[way] * hop, core_num)
        base = half if (way == 0) == (kind == 1) else 0
        return tok.at[origin, pl.ds(pl.multiple_of(base + ck * piece, piece), piece)]

    def sib_msg(way, kind, hop, ck, core_num):
        return to_sib(sib_view(way, kind, hop, ck, core_num), sb_s.at[way, kind, hop - 1, ck], sb_r.at[way, kind, hop - 1, ck])

    def sib_meta(way, hop, core_num):
        return to_sib(meta.at[place(chip - sign[way] * hop, core_num)], sbm_s.at[way, hop - 1], sbm_r.at[way, hop - 1])

    meta_hops = (far, far - 1)

    barrier = pltpu.get_barrier_semaphore()
    for dev in (side[0], side[1], sib):
        pl.semaphore_signal(barrier, inc=1, device_id={'ep': dev}, device_id_type=MESH)
    local = (pltpu.make_async_copy(ids_in, raw.at[0], local_sem.at[0]), pltpu.make_async_copy(slots_in, raw.at[1], local_sem.at[1]),
             pltpu.make_async_copy(gates_in, meta.at[me, pl.ds(top_k, top_k)], local_sem.at[2]))
    bands = [pltpu.make_async_copy(tok_in.at[part_rows(way, 0, ck)], tok.at[me, part_rows(way, 0, ck)], local_sem.at[3 + ck * 2 + way]) for ck in range(AG_CHUNKS) for way in range(2)]
    for copy in local + tuple(bands):
        copy.start()
    pl.semaphore_wait(barrier, 3)

    own_tok = lambda core_num: to_sib(tok.at[place(chip, core_num)], own_s.at[0], own_r.at[0])
    own_meta = lambda core_num: to_sib(meta.at[place(chip, core_num)], own_s.at[1], own_r.at[1])
    for ck in range(AG_CHUNKS):
        for way in range(2):
            bands[ck * 2 + way].wait()
            ag(way, 0, 1, ck, False)[0].start()
        if ck == 0:
            for copy in local:
                copy.wait()
            slot_ids = raw[1]
            meta[me, pl.ds(0, top_k), :] = jnp.where(slot_ids >= 0, raw[0] * cap + slot_ids - me * cap, -1).astype(F32)
    for way in range(2):
        ag_meta(way, 1, False)[0].start()
    own_meta(core).start()
    own_tok(core).start()
    for idx in range(0, n_w, 2):
        load_up(jnp.int32(idx), idx, begin)
    obuf[...] = jnp.zeros_like(obuf)
    for hop in range(1, far + 1):
        for ck in range(AG_CHUNKS):
            for way in range(2):
                ag(way, 0, hop, ck, True)[0].wait_recv()
                if hop < far:
                    ag(way, 0, hop + 1, ck, False)[0].start()
                sib_msg(way, 0, hop, ck, core).start()
        for way in range(2):
            if hop <= meta_hops[way]:
                ag_meta(way, hop, True)[0].wait_recv()
                if hop < meta_hops[way]:
                    ag_meta(way, hop + 1, False)[0].start()
                sib_meta(way, hop, core).start()
        if hop == far - 1:
            for ck in range(AG_CHUNKS):
                for way in range(2):
                    ag(way, 1, 1, ck, False)[0].start()

    def second_half_event(event):
        hop, ck = event // AG_CHUNKS + 1, event % AG_CHUNKS
        for way in range(2):
            ag(way, 1, hop, ck, True)[0].wait_recv()

            @pl.when(hop < far - 1)
            def _():
                ag(way, 1, hop + 1, ck, False)[0].start()
            sib_msg(way, 1, hop, ck, core).start()

    n_events = (far - 1) * AG_CHUNKS
    n_up = n_exp * n_f
    up_events = [(3 * n_up) // 8 - 1, (3 * n_up) // 4 - 1]
    late = n_events - len(up_events)
    down_events = [k * n_d // late for k in range(late)]

    def rs(way, slot, d):
        return pltpu.make_async_remote_copy(ring.at[way, slot, d], ring.at[way, slot + 1, d], rs_s.at[way, slot, d], rs_r.at[way, slot + 1, d], device_id={'ep': side[way]}, device_id_type=MESH)

    def rs_wait(way, slot, d):
        @pl.when(d % PACK == 0)
        def _():
            rs_arrived(way, slot, d // PACK)

    def rs_send(way, slot, d):
        @pl.when(d % PACK == PACK - 1)
        def _():
            rs(way, slot, d // PACK).start()

    def rs_arrived(way, slot, d):
        pltpu.make_async_remote_copy(ring.at[way, slot, d], ring.at[way, slot, d], rs_s.at[way, slot, d], rs_r.at[way, slot, d], device_id={'ep': side[way]}, device_id_type=MESH).wait_recv()

    lane_rows = (pl.ds(0, half), pl.ds(half, half))

    def phase(dist, order, shards, last=False, events=False):
        width = shards // 2
        m_rows = shards * cap

        def shard_place(num):
            which = num % width
            step = dist if width == 1 else dist * (1 - 2 * which)
            return place(chip + step, jnp.where(num < width, core, other))

        def gather(num, carry):
            shard = shard_place(num)
            base = (me * n_exp * cap).astype(F32)
            row_num = lax.broadcasted_iota(jnp.int32, (slots, rows), 0)
            in_exp = row_num % spad
            want = jnp.where(in_exp < cap, (row_num // spad) * cap + in_exp, -7).astype(F32)
            codes = meta[shard, pl.ds(0, top_k), :] - base
            gates = meta[shard, pl.ds(top_k, top_k), :]
            hot = jnp.zeros((slots, rows), F32)
            gate = jnp.zeros((slots, rows), F32)
            for j in range(top_k):
                same = want == codes[j:j + 1, :]
                hot = jnp.where(same, 1.0, hot)
                gate = jnp.where(same, gates[j:j + 1, :], gate)
            slot_gate = jnp.broadcast_to(jnp.sum(gate, axis=1, keepdims=True), (slots, 128))
            first = pl.multiple_of(num * cap, 16)
            for e in range(n_exp):
                sgbuf[e, pl.ds(first, cap), :] = slot_gate[e * spad:e * spad + cap]
            ptbuf[num] = hot.T.astype(BF16)
            pick = hot.astype(BF16)
            for c in range(d_model // COLS):
                got = jnp.dot(pick, tok[shard, :, pl.ds(c * COLS, COLS)], preferred_element_type=F32).astype(BF16)
                for e in range(n_exp):
                    xbuf[e, pl.ds(first, cap), pl.ds(c * COLS, COLS)] = got[e * spad:e * spad + cap]
            return carry

        lax.fori_loop(0, shards, gather, 0)

        def up_step(step, carry):
            idx = step * 2
            slot = idx % n_w
            load_up(idx, slot, finish)
            e, col = step // n_f, pl.multiple_of((step % n_f) * COLS, COLS)
            x = xbuf[e, pl.ds(0, m_rows), :]
            a = jnp.dot(x, wbuf[slot], preferred_element_type=F32)
            u = jnp.dot(x, wbuf[slot + 1], preferred_element_type=F32)
            hbuf[e, pl.ds(0, m_rows), pl.ds(col, COLS)] = (jax.nn.silu(a) * u).astype(BF16)

            @pl.when(idx + n_w < up_loads)
            def _():
                load_up(idx + n_w, slot, begin)

            @pl.when(idx + n_w >= up_loads)
            def _():
                for k in range(2):
                    load_down(idx + n_w + k - up_loads, slot + k, begin)
            if events:
                for k, at in enumerate(up_events):
                    @pl.when(step == at)
                    def _():
                        second_half_event(k)
            return carry

        lax.fori_loop(0, n_exp * n_f, up_step, 0)

        def sib_share(d, waiting=False):
            count = order * n_d + d
            return pltpu.make_async_remote_copy(sib_out.at[d % 2, pl.ds(0, width)], sib_in.at[count % SIB_SLOTS, pl.ds(0, width)], ss_s.at[d % 2], ss_r.at[count % SIB_SLOTS], device_id={'ep': sib}, device_id_type=MESH)

        def close(d):
            count = order * n_d + d
            slot = count % SIB_SLOTS
            sib_share(d).wait_recv()
            mine = lambda i, r: own[d % 2, i, lane_rows[r], :] + sib_in[slot, i, lane_rows[r], :]
            if last:
                for way in range(2):
                    rs_wait(way, a_slot + far, d)
                    rs_wait(way, b_slot + far - 1, d)
                for r in range(2):
                    total = mine(0, r) + ring[r, a_slot + far, d // PACK, d % PACK] + ring[1 - r, b_slot + far - 1, d // PACK, d % PACK]
                    out[lane_rows[r], pl.ds(pl.multiple_of(d * COLS, COLS), COLS)] = total.astype(BF16)
            elif width == 1:
                for way in range(2):
                    ring[way, a_slot, d // PACK, d % PACK] = mine(0, way)
                    rs_send(way, a_slot, d)
            else:
                b_now = b_slot + far - 1 - dist
                a_now = a_slot + far - dist

                @pl.when(dist == far - 1)
                def _():
                    for way in range(2):
                        ring[way, b_slot, d // PACK, d % PACK] = mine(way, 1 - way)

                @pl.when(dist != far - 1)
                def _():
                    for way in range(2):
                        rs_wait(way, b_now, d)
                        ring[way, b_now, d // PACK, d % PACK] += mine(way, 1 - way)
                for way in range(2):
                    rs_send(way, b_now, d)
                for way in range(2):
                    rs_wait(way, a_now, d)
                    ring[way, a_now, d // PACK, d % PACK] += mine(way, way)
                    rs_send(way, a_now, d)

            @pl.when(count < total_chunks - SIB_SLOTS)
            def _():
                pl.semaphore_signal(credit, inc=1, device_id={'ep': sib}, device_id_type=MESH)

        def down_step(d, carry):
            for pair in range(n_exp // 2):
                idx = d * (n_exp // 2) + pair
                slot = (up_loads + idx) % n_w
                load_down(idx, slot, finish)
                for k in range(2):
                    e = pair * 2 + k
                    o = jnp.dot(hbuf[e, pl.ds(0, m_rows), :], wbuf[slot, pl.ds(k * d_ff, d_ff), :], preferred_element_type=F32)
                    g = sgbuf[e, pl.ds(0, m_rows), :]
                    o = o * jnp.concatenate([g] * (COLS // 128), axis=1)
                    for p in range(3):
                        cut = o.astype(BF16)
                        o = o - cut.astype(F32)
                        for i in range(shards):
                            obuf[i, pl.ds(p * slots + e * spad, cap), :] = cut[i * cap:(i + 1) * cap]

                @pl.when(up_loads + idx + n_w < loads)
                def _():
                    load_down(idx + n_w, slot, begin)
                if not last:
                    @pl.when((up_loads + idx + n_w >= loads) & ((up_loads + idx + n_w - loads) % 2 == 1))
                    def _():
                        load_up(up_loads + idx + n_w - loads - 1, slot - 1, begin)

            @pl.when(d >= 2)
            def _():
                sib_share(d).wait_send()

            @pl.when(order * n_d + d >= SIB_SLOTS)
            def _():
                pl.semaphore_wait(credit, 1)
            for i in list(range(width, shards)) + list(range(width)):
                pt = ptbuf[i]
                share = jnp.dot(pt, obuf[i, pl.ds(0, slots), :], preferred_element_type=F32)
                for p in range(1, 3):
                    share += jnp.dot(pt, obuf[i, pl.ds(p * slots, slots), :], preferred_element_type=F32)
                if i >= width:
                    sib_out[d % 2, i - width] = share
                else:
                    own[d % 2, i] = share
                if i == shards - 1:
                    sib_share(d).start()

            @pl.when(d >= 1)
            def _():
                close(d - 1)
            if events:
                for k, at in enumerate(down_events):
                    @pl.when(d == at)
                    def _():
                        second_half_event(len(up_events) + k)
            return carry

        lax.fori_loop(0, n_d, down_step, 0)
        close(jnp.int32(n_d - 1))
        for d in range(n_d - 2, n_d):
            sib_share(d).wait_send()

    for way in range(2):
        if far <= meta_hops[way]:
            sib_meta(way, far, other).wait_recv()
        for ck in range(AG_CHUNKS):
            sib_msg(way, 0, far, ck, other).wait_recv()
    phase(far, 0, 2, events=True)

    def middle(order, carry):
        dist = far - order
        for way in range(2):
            sib_meta(way, dist, other).wait_recv()
            for kind in range(2):
                for ck in range(AG_CHUNKS):
                    sib_msg(way, kind, dist, ck, other).wait_recv()
        phase(dist, order, 4)
        return carry

    lax.fori_loop(1, far, middle, 0)
    own_meta(other).wait_recv()
    own_tok(other).wait_recv()
    phase(0, far, 2, last=True)

    own_meta(core).wait_send()
    own_tok(core).wait_send()
    for way in range(2):
        for hop in range(1, far + 1):
            if hop <= meta_hops[way]:
                ag_meta(way, hop, False)[0].wait_send()
                sib_meta(way, hop, core).wait_send()
            for kind in range(2):
                if hop <= far - kind:
                    for ck in range(AG_CHUNKS):
                        ag(way, kind, hop, ck, False)[0].wait_send()
                        sib_msg(way, kind, hop, ck, core).wait_send()

        def drain(d, carry):
            for slot in list(range(a_slot, a_slot + far)) + list(range(b_slot, b_slot + far - 1)):
                rs(way, slot, d).wait_send()
            return carry
        lax.fori_loop(0, n_d // PACK, drain, 0)


def group_layer(n, tokens, ids, gates, slot_ids, w_gate, w_up, w_down, cap):
    rows, d_model = tokens.shape
    top_k = ids.shape[0]
    n_exp, _, d_ff = w_gate.shape
    far = n // 4
    spad = (cap + 63) // 64 * 64
    slots = n_exp * spad
    n_d = d_model // COLS
    loads = 2 * n_exp * d_ff // COLS + n_d * n_exp // 2
    n_w = 8 if loads % 8 == 0 else 4
    any_spec = pl.BlockSpec(memory_space=pl.ANY)
    dma = pltpu.SemaphoreType.DMA
    ag_shape = (2, 2, far, AG_CHUNKS)
    return pl.pallas_call(
        functools.partial(moe_kernel, (n, cap, spad, n_w)),
        out_shape=pltpu.VMEM((rows, d_model), BF16),
        in_specs=[any_spec] * 7,
        out_specs=pl.BlockSpec(memory_space=pltpu.VMEM),
        scratch_shapes=[
            pltpu.VMEM((n, rows, d_model), BF16),
            pltpu.VMEM((n, 2 * top_k, rows), F32),
            pltpu.VMEM((2, top_k, rows), jnp.int32),
            pltpu.VMEM((2, 2 * far + 1, n_d // PACK, PACK, rows // 2, COLS), F32),
            pltpu.VMEM((SIB_SLOTS, 2, rows, COLS), F32),
            pltpu.VMEM((2, 2, rows, COLS), F32),
            pltpu.VMEM((2, 2, rows, COLS), F32),
            pltpu.VMEM((n_w, d_model, COLS), BF16),
            pltpu.VMEM((n_exp, 4 * cap, d_model), BF16),
            pltpu.VMEM((n_exp, 4 * cap, d_ff), BF16),
            pltpu.VMEM((4, 3 * slots, COLS), BF16),
            pltpu.VMEM((4, rows, slots), BF16),
            pltpu.VMEM((n_exp, 4 * cap, 128), F32),
            dma((3 + 2 * AG_CHUNKS,)), dma((n_w, 2)),
            dma(ag_shape), dma(ag_shape), dma((2, far)), dma((2, far)),
            dma(ag_shape), dma(ag_shape), dma((2, far)), dma((2, far)),
            dma((2,)), dma((2,)),
            dma((2, 2 * far + 1, n_d // PACK)), dma((2, 2 * far + 1, n_d // PACK)),
            dma((2,)), dma((SIB_SLOTS,)),
            pltpu.SemaphoreType.REGULAR,
        ],
        compiler_params=pltpu.CompilerParams(collective_id=0, has_side_effects=True, vmem_limit_bytes=58 << 20),
    )(tokens, ids, gates, slot_ids, w_gate, w_up, w_down)


def solution(mesh):
    group_size = mesh.shape['ep']
    row_spec = P(('dp', 'ep'), None)
    expert_spec = P('ep', None, None)

    def per_device(tokens, expert_ids, gate_wts, slot_ids, w_gate, w_up, w_down):
        tok_dev, top_k = expert_ids.shape
        cap = CAP_NUM * tok_dev * top_k // (CAP_DEN * w_gate.shape[0] * group_size)
        return group_layer(group_size, tokens, expert_ids.T, gate_wts.T, slot_ids.T, w_gate, w_up, w_down, cap)

    return jax.shard_map(per_device, mesh=mesh, in_specs=(row_spec, row_spec, row_spec, row_spec, expert_spec, expert_spec, expert_spec), out_specs=row_spec, check_vma=False)
```

```python
import functools

import jax
import jax.numpy as jnp
from jax import lax
from jax.experimental import pallas as pl
from jax.experimental.pallas import tpu as pltpu
from jax.sharding import PartitionSpec as P

CAP_NUM = 3
CAP_DEN = 2
COLS = 256
AG_CHUNKS = 2
SIB_SLOTS = 4
PACK = 2
MESH = pl.DeviceIdType.MESH
BF16 = jnp.bfloat16
F32 = jnp.float32


def moe_kernel(cfg, tok_in, ids_in, gates_in, slots_in, wg, wu, wd, out,
               tok, meta, raw, ring, sib_in, sib_out, own, wbuf, xbuf, hbuf, obuf, ptbuf, sgbuf,
               local_sem, w_sem, ag_s, ag_r, agm_s, agm_r, sb_s, sb_r, sbm_s, sbm_r, own_s, own_r,
               rs_s, rs_r, ss_s, ss_r, credit):
    n, cap, spad, n_w = cfg
    rows, d_model = tok_in.shape
    top_k = ids_in.shape[0]
    n_exp, _, d_ff = wg.shape
    chips = n // 2
    far = chips // 2
    half = rows // 2
    piece = half // AG_CHUNKS
    n_d = d_model // COLS
    n_f = d_ff // COLS
    slots = n_exp * spad
    up_loads = 2 * n_exp * n_f
    loads = up_loads + n_d * n_exp // 2
    total_chunks = (far + 1) * n_d
    a_slot, b_slot = 0, far + 1

    me = lax.axis_index('ep')
    chip, core = me // 2, me % 2
    other = 1 - core

    def place(chip_num, core_num):
        return ((chip_num + chips) % chips) * 2 + core_num

    sib = chip * 2 + other
    side = (place(chip + 1, core), place(chip - 1, core))
    sign = (1, -1)

    def load_up(idx, slot, start):
        step = idx // 2
        exp_num, col = step // n_f, pl.multiple_of((step % n_f) * COLS, COLS)
        start(pltpu.make_async_copy(wg.at[exp_num, :, pl.ds(col, COLS)], wbuf.at[slot], w_sem.at[slot, 0]))
        start(pltpu.make_async_copy(wu.at[exp_num, :, pl.ds(col, COLS)], wbuf.at[slot + 1], w_sem.at[slot + 1, 0]))

    def load_down(idx, slot, start):
        col, pair = pl.multiple_of((idx // (n_exp // 2)) * COLS, COLS), idx % (n_exp // 2)
        for k in range(2):
            start(pltpu.make_async_copy(wd.at[pair * 2 + k, :, pl.ds(col, COLS)], wbuf.at[slot, pl.ds(k * d_ff, d_ff)], w_sem.at[slot, k]))

    begin = lambda copy: copy.start()
    finish = lambda copy: copy.wait()

    def part_rows(way, kind, ck):
        upper = (way == 0) == (kind == 1)
        return pl.ds((half if upper else 0) + ck * piece, piece)

    def ag(way, kind, hop, ck, arriving):
        origin = place(chip - sign[way] * (hop if arriving else hop - 1), core)
        if isinstance(ck, int):
            view = tok.at[origin, part_rows(way, kind, ck)]
        else:
            base = half if (way == 0) == (kind == 1) else 0
            view = tok.at[origin, pl.ds(pl.multiple_of(base + ck * piece, piece), piece)]
        copy = pltpu.make_async_remote_copy(view, view, ag_s.at[way, kind, hop - 1, ck], ag_r.at[way, kind, hop - 1, ck], device_id={'ep': side[way]}, device_id_type=MESH)
        return copy, origin, view

    def ag_meta(way, hop, arriving):
        origin = place(chip - sign[way] * (hop if arriving else hop - 1), core)
        view = meta.at[origin]
        copy = pltpu.make_async_remote_copy(view, view, agm_s.at[way, hop - 1], agm_r.at[way, hop - 1], device_id={'ep': side[way]}, device_id_type=MESH)
        return copy, origin, view

    def to_sib(view, send_sem, recv_sem):
        return pltpu.make_async_remote_copy(view, view, send_sem, recv_sem, device_id={'ep': sib}, device_id_type=MESH)

    def sib_view(way, kind, hop, ck, core_num):
        origin = place(chip - sign[way] * hop, core_num)
        base = half if (way == 0) == (kind == 1) else 0
        return tok.at[origin, pl.ds(pl.multiple_of(base + ck * piece, piece), piece)]

    def sib_msg(way, kind, hop, ck, core_num):
        return to_sib(sib_view(way, kind, hop, ck, core_num), sb_s.at[way, kind, hop - 1, ck], sb_r.at[way, kind, hop - 1, ck])

    def sib_meta(way, hop, core_num):
        return to_sib(meta.at[place(chip - sign[way] * hop, core_num)], sbm_s.at[way, hop - 1], sbm_r.at[way, hop - 1])

    meta_hops = (far, far - 1)

    barrier = pltpu.get_barrier_semaphore()
    for dev in (side[0], side[1], sib):
        pl.semaphore_signal(barrier, inc=1, device_id={'ep': dev}, device_id_type=MESH)
    local = (pltpu.make_async_copy(ids_in, raw.at[0], local_sem.at[0]), pltpu.make_async_copy(slots_in, raw.at[1], local_sem.at[1]),
             pltpu.make_async_copy(gates_in, meta.at[me, pl.ds(top_k, top_k)], local_sem.at[2]))
    bands = [pltpu.make_async_copy(tok_in.at[part_rows(way, 0, ck)], tok.at[me, part_rows(way, 0, ck)], local_sem.at[3 + ck * 2 + way]) for ck in range(AG_CHUNKS) for way in range(2)]
    for copy in local + tuple(bands):
        copy.start()
    pl.semaphore_wait(barrier, 3)

    own_tok = lambda core_num: to_sib(tok.at[place(chip, core_num)], own_s.at[0], own_r.at[0])
    own_meta = lambda core_num: to_sib(meta.at[place(chip, core_num)], own_s.at[1], own_r.at[1])
    for ck in range(AG_CHUNKS):
        for way in range(2):
            bands[ck * 2 + way].wait()
            ag(way, 0, 1, ck, False)[0].start()
        if ck == 0:
            for copy in local:
                copy.wait()
            slot_ids = raw[1]
            meta[me, pl.ds(0, top_k), :] = jnp.where(slot_ids >= 0, raw[0] * cap + slot_ids - me * cap, -1).astype(F32)
    for way in range(2):
        ag_meta(way, 1, False)[0].start()
    own_meta(core).start()
    own_tok(core).start()
    for idx in range(0, n_w, 2):
        load_up(jnp.int32(idx), idx, begin)
    obuf[...] = jnp.zeros_like(obuf)
    for hop in range(1, far + 1):
        for ck in range(AG_CHUNKS):
            for way in range(2):
                ag(way, 0, hop, ck, True)[0].wait_recv()
                if hop < far:
                    ag(way, 0, hop + 1, ck, False)[0].start()
                sib_msg(way, 0, hop, ck, core).start()
        for way in range(2):
            if hop <= meta_hops[way]:
                ag_meta(way, hop, True)[0].wait_recv()
                if hop < meta_hops[way]:
                    ag_meta(way, hop + 1, False)[0].start()
                sib_meta(way, hop, core).start()
        if hop == far - 1:
            for ck in range(AG_CHUNKS):
                for way in range(2):
                    ag(way, 1, 1, ck, False)[0].start()

    def second_half_event(event):
        hop, ck = event // AG_CHUNKS + 1, event % AG_CHUNKS
        for way in range(2):
            ag(way, 1, hop, ck, True)[0].wait_recv()

            @pl.when(hop < far - 1)
            def _():
                ag(way, 1, hop + 1, ck, False)[0].start()
            sib_msg(way, 1, hop, ck, core).start()

    n_events = (far - 1) * AG_CHUNKS
    n_up = n_exp * n_f
    up_events = [(k + 1) * n_up // (n_events - 2) - 1 for k in range(n_events - 2)]
    down_events = [n_d // 2 - 1, n_d - 1]

    def rs(way, slot, d):
        return pltpu.make_async_remote_copy(ring.at[way, slot, d], ring.at[way, slot + 1, d], rs_s.at[way, slot, d], rs_r.at[way, slot + 1, d], device_id={'ep': side[way]}, device_id_type=MESH)

    def rs_wait(way, slot, d):
        @pl.when(d % PACK == 0)
        def _():
            rs_arrived(way, slot, d // PACK)

    def rs_send(way, slot, d):
        @pl.when(d % PACK == PACK - 1)
        def _():
            rs(way, slot, d // PACK).start()

    def rs_arrived(way, slot, d):
        pltpu.make_async_remote_copy(ring.at[way, slot, d], ring.at[way, slot, d], rs_s.at[way, slot, d], rs_r.at[way, slot, d], device_id={'ep': side[way]}, device_id_type=MESH).wait_recv()

    lane_rows = (pl.ds(0, half), pl.ds(half, half))

    def phase(dist, order, shards, last=False, events=False):
        width = shards // 2
        m_rows = shards * cap

        def shard_place(num):
            which = num % width
            step = dist if width == 1 else dist * (1 - 2 * which)
            return place(chip + step, jnp.where(num < width, core, other))

        def gather(num, carry):
            shard = shard_place(num)
            base = (me * n_exp * cap).astype(F32)
            row_num = lax.broadcasted_iota(jnp.int32, (slots, rows), 0)
            in_exp = row_num % spad
            want = jnp.where(in_exp < cap, (row_num // spad) * cap + in_exp, -7).astype(F32)
            codes = meta[shard, pl.ds(0, top_k), :] - base
            gates = meta[shard, pl.ds(top_k, top_k), :]
            hot = jnp.zeros((slots, rows), F32)
            gate = jnp.zeros((slots, rows), F32)
            for j in range(top_k):
                same = want == codes[j:j + 1, :]
                hot = jnp.where(same, 1.0, hot)
                gate = jnp.where(same, gates[j:j + 1, :], gate)
            slot_gate = jnp.broadcast_to(jnp.sum(gate, axis=1, keepdims=True), (slots, 128))
            first = pl.multiple_of(num * cap, 16)
            for e in range(n_exp):
                sgbuf[e, pl.ds(first, cap), :] = slot_gate[e * spad:e * spad + cap]
            ptbuf[num] = hot.T.astype(BF16)
            pick = hot.astype(BF16)
            for c in range(d_model // COLS):
                got = jnp.dot(pick, tok[shard, :, pl.ds(c * COLS, COLS)], preferred_element_type=F32).astype(BF16)
                for e in range(n_exp):
                    xbuf[e, pl.ds(first, cap), pl.ds(c * COLS, COLS)] = got[e * spad:e * spad + cap]
            return carry

        lax.fori_loop(0, shards, gather, 0)

        def up_step(step, carry):
            idx = step * 2
            slot = idx % n_w
            load_up(idx, slot, finish)
            e, col = step // n_f, pl.multiple_of((step % n_f) * COLS, COLS)
            x = xbuf[e, pl.ds(0, m_rows), :]
            a = jnp.dot(x, wbuf[slot], preferred_element_type=F32)
            u = jnp.dot(x, wbuf[slot + 1], preferred_element_type=F32)
            hbuf[e, pl.ds(0, m_rows), pl.ds(col, COLS)] = (jax.nn.silu(a) * u).astype(BF16)

            @pl.when(idx + n_w < up_loads)
            def _():
                load_up(idx + n_w, slot, begin)

            @pl.when(idx + n_w >= up_loads)
            def _():
                for k in range(2):
                    load_down(idx + n_w + k - up_loads, slot + k, begin)
            if events:
                for k, at in enumerate(up_events):
                    @pl.when(step == at)
                    def _():
                        second_half_event(k)
            return carry

        lax.fori_loop(0, n_exp * n_f, up_step, 0)

        def sib_share(d, waiting=False):
            count = order * n_d + d
            return pltpu.make_async_remote_copy(sib_out.at[d % 2, pl.ds(0, width)], sib_in.at[count % SIB_SLOTS, pl.ds(0, width)], ss_s.at[d % 2], ss_r.at[count % SIB_SLOTS], device_id={'ep': sib}, device_id_type=MESH)

        def close(d):
            count = order * n_d + d
            slot = count % SIB_SLOTS
            sib_share(d).wait_recv()
            mine = lambda i, r: own[d % 2, i, lane_rows[r], :] + sib_in[slot, i, lane_rows[r], :]
            if last:
                for way in range(2):
                    rs_wait(way, a_slot + far, d)
                    rs_wait(way, b_slot + far - 1, d)
                for r in range(2):
                    total = mine(0, r) + ring[r, a_slot + far, d // PACK, d % PACK] + ring[1 - r, b_slot + far - 1, d // PACK, d % PACK]
                    out[lane_rows[r], pl.ds(pl.multiple_of(d * COLS, COLS), COLS)] = total.astype(BF16)
            elif width == 1:
                for way in range(2):
                    ring[way, a_slot, d // PACK, d % PACK] = mine(0, way)
                    rs_send(way, a_slot, d)
            else:
                b_now = b_slot + far - 1 - dist
                a_now = a_slot + far - dist

                @pl.when(dist == far - 1)
                def _():
                    for way in range(2):
                        ring[way, b_slot, d // PACK, d % PACK] = mine(way, 1 - way)

                @pl.when(dist != far - 1)
                def _():
                    for way in range(2):
                        rs_wait(way, b_now, d)
                        ring[way, b_now, d // PACK, d % PACK] += mine(way, 1 - way)
                for way in range(2):
                    rs_send(way, b_now, d)
                for way in range(2):
                    rs_wait(way, a_now, d)
                    ring[way, a_now, d // PACK, d % PACK] += mine(way, way)
                    rs_send(way, a_now, d)

            @pl.when(count < total_chunks - SIB_SLOTS)
            def _():
                pl.semaphore_signal(credit, inc=1, device_id={'ep': sib}, device_id_type=MESH)

        def down_step(d, carry):
            for pair in range(n_exp // 2):
                idx = d * (n_exp // 2) + pair
                slot = (up_loads + idx) % n_w
                load_down(idx, slot, finish)
                for k in range(2):
                    e = pair * 2 + k
                    o = jnp.dot(hbuf[e, pl.ds(0, m_rows), :], wbuf[slot, pl.ds(k * d_ff, d_ff), :], preferred_element_type=F32)
                    g = sgbuf[e, pl.ds(0, m_rows), :]
                    o = o * jnp.concatenate([g] * (COLS // 128), axis=1)
                    for p in range(3):
                        cut = o.astype(BF16)
                        o = o - cut.astype(F32)
                        for i in range(shards):
                            obuf[i, pl.ds(p * slots + e * spad, cap), :] = cut[i * cap:(i + 1) * cap]

                @pl.when(up_loads + idx + n_w < loads)
                def _():
                    load_down(idx + n_w, slot, begin)
                if not last:
                    @pl.when((up_loads + idx + n_w >= loads) & ((up_loads + idx + n_w - loads) % 2 == 1))
                    def _():
                        load_up(up_loads + idx + n_w - loads - 1, slot - 1, begin)

            @pl.when(d >= 2)
            def _():
                sib_share(d).wait_send()

            @pl.when(order * n_d + d >= SIB_SLOTS)
            def _():
                pl.semaphore_wait(credit, 1)
            for i in list(range(width, shards)) + list(range(width)):
                pt = ptbuf[i]
                share = jnp.dot(pt, obuf[i, pl.ds(0, slots), :], preferred_element_type=F32)
                for p in range(1, 3):
                    share += jnp.dot(pt, obuf[i, pl.ds(p * slots, slots), :], preferred_element_type=F32)
                if i >= width:
                    sib_out[d % 2, i - width] = share
                else:
                    own[d % 2, i] = share
                if i == shards - 1:
                    sib_share(d).start()

            @pl.when(d >= 1)
            def _():
                close(d - 1)
            if events:
                for k, at in enumerate(down_events):
                    @pl.when(d == at)
                    def _():
                        second_half_event(len(up_events) + k)
            return carry

        lax.fori_loop(0, n_d, down_step, 0)
        close(jnp.int32(n_d - 1))
        for d in range(n_d - 2, n_d):
            sib_share(d).wait_send()

    for way in range(2):
        if far <= meta_hops[way]:
            sib_meta(way, far, other).wait_recv()
        for ck in range(AG_CHUNKS):
            sib_msg(way, 0, far, ck, other).wait_recv()
    phase(far, 0, 2, events=True)

    def middle(order, carry):
        dist = far - order
        for way in range(2):
            sib_meta(way, dist, other).wait_recv()
            for kind in range(2):
                for ck in range(AG_CHUNKS):
                    sib_msg(way, kind, dist, ck, other).wait_recv()
        phase(dist, order, 4)
        return carry

    lax.fori_loop(1, far, middle, 0)
    own_meta(other).wait_recv()
    own_tok(other).wait_recv()
    phase(0, far, 2, last=True)

    own_meta(core).wait_send()
    own_tok(core).wait_send()
    for way in range(2):
        for hop in range(1, far + 1):
            if hop <= meta_hops[way]:
                ag_meta(way, hop, False)[0].wait_send()
                sib_meta(way, hop, core).wait_send()
            for kind in range(2):
                if hop <= far - kind:
                    for ck in range(AG_CHUNKS):
                        ag(way, kind, hop, ck, False)[0].wait_send()
                        sib_msg(way, kind, hop, ck, core).wait_send()

        def drain(d, carry):
            for slot in list(range(a_slot, a_slot + far)) + list(range(b_slot, b_slot + far - 1)):
                rs(way, slot, d).wait_send()
            return carry
        lax.fori_loop(0, n_d // PACK, drain, 0)


def group_layer(n, tokens, ids, gates, slot_ids, w_gate, w_up, w_down, cap):
    rows, d_model = tokens.shape
    top_k = ids.shape[0]
    n_exp, _, d_ff = w_gate.shape
    far = n // 4
    spad = (cap + 63) // 64 * 64
    slots = n_exp * spad
    n_d = d_model // COLS
    loads = 2 * n_exp * d_ff // COLS + n_d * n_exp // 2
    n_w = next(k for k in (12, 8, 6, 4) if loads % k == 0 and k <= n_d * n_exp // 2)
    any_spec = pl.BlockSpec(memory_space=pl.ANY)
    dma = pltpu.SemaphoreType.DMA
    ag_shape = (2, 2, far, AG_CHUNKS)
    return pl.pallas_call(
        functools.partial(moe_kernel, (n, cap, spad, n_w)),
        out_shape=pltpu.VMEM((rows, d_model), BF16),
        in_specs=[any_spec] * 7,
        out_specs=pl.BlockSpec(memory_space=pltpu.VMEM),
        scratch_shapes=[
            pltpu.VMEM((n, rows, d_model), BF16),
            pltpu.VMEM((n, 2 * top_k, rows), F32),
            pltpu.VMEM((2, top_k, rows), jnp.int32),
            pltpu.VMEM((2, 2 * far + 1, n_d // PACK, PACK, rows // 2, COLS), F32),
            pltpu.VMEM((SIB_SLOTS, 2, rows, COLS), F32),
            pltpu.VMEM((2, 2, rows, COLS), F32),
            pltpu.VMEM((2, 2, rows, COLS), F32),
            pltpu.VMEM((n_w, d_model, COLS), BF16),
            pltpu.VMEM((n_exp, 4 * cap, d_model), BF16),
            pltpu.VMEM((n_exp, 4 * cap, d_ff), BF16),
            pltpu.VMEM((4, 3 * slots, COLS), BF16),
            pltpu.VMEM((4, rows, slots), BF16),
            pltpu.VMEM((n_exp, 4 * cap, 128), F32),
            dma((3 + 2 * AG_CHUNKS,)), dma((n_w, 2)),
            dma(ag_shape), dma(ag_shape), dma((2, far)), dma((2, far)),
            dma(ag_shape), dma(ag_shape), dma((2, far)), dma((2, far)),
            dma((2,)), dma((2,)),
            dma((2, 2 * far + 1, n_d // PACK)), dma((2, 2 * far + 1, n_d // PACK)),
            dma((2,)), dma((SIB_SLOTS,)),
            pltpu.SemaphoreType.REGULAR,
        ],
        compiler_params=pltpu.CompilerParams(collective_id=0, has_side_effects=True, vmem_limit_bytes=61 << 20),
    )(tokens, ids, gates, slot_ids, w_gate, w_up, w_down)


def solution(mesh):
    group_size = mesh.shape['ep']
    row_spec = P(('dp', 'ep'), None)
    expert_spec = P('ep', None, None)

    def per_device(tokens, expert_ids, gate_wts, slot_ids, w_gate, w_up, w_down):
        tok_dev, top_k = expert_ids.shape
        cap = CAP_NUM * tok_dev * top_k // (CAP_DEN * w_gate.shape[0] * group_size)
        return group_layer(group_size, tokens, expert_ids.T, gate_wts.T, slot_ids.T, w_gate, w_up, w_down, cap)

    return jax.shard_map(per_device, mesh=mesh, in_specs=(row_spec, row_spec, row_spec, row_spec, expert_spec, expert_spec, expert_spec), out_specs=row_spec, check_vma=False)
```

```python
import functools

import jax
import jax.numpy as jnp
from jax import lax
from jax.experimental import pallas as pl
from jax.experimental.pallas import tpu as pltpu
from jax.sharding import PartitionSpec as P

CAP_NUM = 3
CAP_DEN = 2
COLS = 256
AG_CHUNKS = 2
SIB_SLOTS = 4
PACK = 2
MESH = pl.DeviceIdType.MESH
BF16 = jnp.bfloat16
F32 = jnp.float32


def moe_kernel(cfg, tok_in, ids_in, gates_in, slots_in, wg, wu, wd, out,
               tok, meta, raw, ring, sib_in, sib_out, own, wbuf, xbuf, hbuf, obuf, ptbuf, sgbuf,
               local_sem, w_sem, ag_s, ag_r, agm_s, agm_r, sb_s, sb_r, sbm_s, sbm_r, own_s, own_r, guest_s, guest_r,
               rs_s, rs_r, ss_s, ss_r, credit):
    n, cap, spad, n_w = cfg
    rows, d_model = tok_in.shape
    top_k = ids_in.shape[0]
    n_exp, _, d_ff = wg.shape
    chips = n // 2
    far = chips // 2
    half = rows // 2
    piece = half // AG_CHUNKS
    n_d = d_model // COLS
    n_f = d_ff // COLS
    slots = n_exp * spad
    up_loads = 2 * n_exp * n_f
    loads = up_loads + n_d * n_exp // 2
    total_chunks = (far + 1) * n_d
    a_slot, b_slot = 0, far + 1

    me = lax.axis_index('ep')
    chip, core = me // 2, me % 2
    other = 1 - core

    def place(chip_num, core_num):
        return ((chip_num + chips) % chips) * 2 + core_num

    sib = chip * 2 + other
    side = (place(chip + 1, core), place(chip - 1, core))
    sign = (1, -1)

    def load_up(idx, slot, start):
        step = idx // 2
        exp_num, col = step // n_f, pl.multiple_of((step % n_f) * COLS, COLS)
        start(pltpu.make_async_copy(wg.at[exp_num, :, pl.ds(col, COLS)], wbuf.at[slot], w_sem.at[slot, 0]))
        start(pltpu.make_async_copy(wu.at[exp_num, :, pl.ds(col, COLS)], wbuf.at[slot + 1], w_sem.at[slot + 1, 0]))

    def load_down(idx, slot, start):
        col, pair = pl.multiple_of((idx // (n_exp // 2)) * COLS, COLS), idx % (n_exp // 2)
        for k in range(2):
            start(pltpu.make_async_copy(wd.at[pair * 2 + k, :, pl.ds(col, COLS)], wbuf.at[slot, pl.ds(k * d_ff, d_ff)], w_sem.at[slot, k]))

    begin = lambda copy: copy.start()
    finish = lambda copy: copy.wait()

    def part_rows(way, kind, ck):
        upper = (way == 0) == (kind == 1)
        return pl.ds((half if upper else 0) + ck * piece, piece)

    def ag(way, kind, hop, ck, arriving):
        origin = place(chip - sign[way] * (hop if arriving else hop - 1), core)
        if isinstance(ck, int):
            view = tok.at[origin, part_rows(way, kind, ck)]
        else:
            base = half if (way == 0) == (kind == 1) else 0
            view = tok.at[origin, pl.ds(pl.multiple_of(base + ck * piece, piece), piece)]
        copy = pltpu.make_async_remote_copy(view, view, ag_s.at[way, kind, hop - 1, ck], ag_r.at[way, kind, hop - 1, ck], device_id={'ep': side[way]}, device_id_type=MESH)
        return copy, origin, view

    def ag_meta(way, hop, arriving):
        origin = place(chip - sign[way] * (hop if arriving else hop - 1), core)
        view = meta.at[origin]
        copy = pltpu.make_async_remote_copy(view, view, agm_s.at[way, hop - 1], agm_r.at[way, hop - 1], device_id={'ep': side[way]}, device_id_type=MESH)
        return copy, origin, view

    def to_sib(view, send_sem, recv_sem):
        return pltpu.make_async_remote_copy(view, view, send_sem, recv_sem, device_id={'ep': sib}, device_id_type=MESH)

    def sib_view(way, kind, hop, ck, core_num):
        origin = place(chip - sign[way] * hop, core_num)
        base = half if (way == 0) == (kind == 1) else 0
        return tok.at[origin, pl.ds(pl.multiple_of(base + ck * piece, piece), piece)]

    def sib_msg(way, kind, hop, ck, core_num):
        return to_sib(sib_view(way, kind, hop, ck, core_num), sb_s.at[way, kind, hop - 1, ck], sb_r.at[way, kind, hop - 1, ck])

    def sib_meta(way, hop, core_num):
        return to_sib(meta.at[place(chip - sign[way] * hop, core_num)], sbm_s.at[way, hop - 1], sbm_r.at[way, hop - 1])

    meta_hops = (far, far - 1)
    swap_ck = AG_CHUNKS - 1

    def split_rows(way, num):
        return pl.ds((0 if way == 0 else half) + swap_ck * piece + num * (piece // 2), piece // 2)

    def stay(way, arriving):
        origin = place(chip - sign[way] * (far if arriving else far - 1), 1)
        view = tok.at[origin, split_rows(way, 0)]
        return pltpu.make_async_remote_copy(view, view, ag_s.at[way, 0, far - 1, swap_ck], ag_r.at[way, 0, far - 1, swap_ck], device_id={'ep': side[way]}, device_id_type=MESH)

    def stay_sib(way):
        origin = place(chip - sign[way] * far, 1)
        return to_sib(tok.at[origin, split_rows(way, 0)], sb_s.at[way, 0, far - 1, swap_ck], sb_r.at[way, 0, far - 1, swap_ck])

    def guest(way, arriving):
        origin = place(chip - sign[way] * (far if arriving else far - 1), 1)
        view = tok.at[origin, split_rows(way, 1)]
        return pltpu.make_async_remote_copy(view, view, guest_s.at[way, 0], guest_r.at[way, 0], device_id={'ep': side[way]}, device_id_type=MESH)

    def guest_sib(way):
        origin = place(chip - sign[way] * far, 1)
        return to_sib(tok.at[origin, split_rows(way, 1)], guest_s.at[way, 1], guest_r.at[way, 1])

    barrier = pltpu.get_barrier_semaphore()
    for dev in (side[0], side[1], sib):
        pl.semaphore_signal(barrier, inc=1, device_id={'ep': dev}, device_id_type=MESH)
    local = (pltpu.make_async_copy(ids_in, raw.at[0], local_sem.at[0]), pltpu.make_async_copy(slots_in, raw.at[1], local_sem.at[1]),
             pltpu.make_async_copy(gates_in, meta.at[me, pl.ds(top_k, top_k)], local_sem.at[2]))
    bands = [pltpu.make_async_copy(tok_in.at[part_rows(way, 0, ck)], tok.at[me, part_rows(way, 0, ck)], local_sem.at[3 + ck * 2 + way]) for ck in range(AG_CHUNKS) for way in range(2)]
    for copy in local + tuple(bands):
        copy.start()
    pl.semaphore_wait(barrier, 3)

    own_tok = lambda core_num: to_sib(tok.at[place(chip, core_num)], own_s.at[0], own_r.at[0])
    own_meta = lambda core_num: to_sib(meta.at[place(chip, core_num)], own_s.at[1], own_r.at[1])
    for ck in range(AG_CHUNKS):
        for way in range(2):
            bands[ck * 2 + way].wait()
            ag(way, 0, 1, ck, False)[0].start()
        if ck == 0:
            for copy in local:
                copy.wait()
            slot_ids = raw[1]
            meta[me, pl.ds(0, top_k), :] = jnp.where(slot_ids >= 0, raw[0] * cap + slot_ids - me * cap, -1).astype(F32)
    for way in range(2):
        ag_meta(way, 1, False)[0].start()
    own_meta(core).start()
    own_tok(core).start()
    for idx in range(0, n_w, 2):
        load_up(jnp.int32(idx), idx, begin)
    obuf[...] = jnp.zeros_like(obuf)
    for hop in range(1, far + 1):
        for ck in range(AG_CHUNKS):
            for way in range(2):
                if hop == far and ck == swap_ck:
                    @pl.when(core == 0)
                    def _():
                        ag(way, 0, hop, ck, True)[0].wait_recv()
                        sib_msg(way, 0, hop, ck, core).start()
                        guest(way, True).wait_recv()
                        guest_sib(way).start()

                    @pl.when(core == 1)
                    def _():
                        stay(way, True).wait_recv()
                        stay_sib(way).start()
                    continue
                ag(way, 0, hop, ck, True)[0].wait_recv()
                if hop + 1 == far and ck == swap_ck:
                    sib_msg(way, 0, hop, ck, core).start()

                    @pl.when(core == 0)
                    def _():
                        ag(way, 0, hop + 1, ck, False)[0].start()
                        sib_msg(way, 0, hop, ck, other).wait_recv()
                        guest(way, False).start()

                    @pl.when(core == 1)
                    def _():
                        stay(way, False).start()
                    continue
                if hop < far:
                    ag(way, 0, hop + 1, ck, False)[0].start()
                sib_msg(way, 0, hop, ck, core).start()
        for way in range(2):
            if hop <= meta_hops[way]:
                ag_meta(way, hop, True)[0].wait_recv()
                if hop < meta_hops[way]:
                    ag_meta(way, hop + 1, False)[0].start()
                sib_meta(way, hop, core).start()
        if hop == far - 1:
            for ck in range(AG_CHUNKS):
                for way in range(2):
                    ag(way, 1, 1, ck, False)[0].start()

    def second_half_event(event):
        hop, ck = event // AG_CHUNKS + 1, event % AG_CHUNKS
        for way in range(2):
            ag(way, 1, hop, ck, True)[0].wait_recv()

            @pl.when(hop < far - 1)
            def _():
                ag(way, 1, hop + 1, ck, False)[0].start()
            sib_msg(way, 1, hop, ck, core).start()

    n_events = (far - 1) * AG_CHUNKS

    def rs(way, slot, d):
        return pltpu.make_async_remote_copy(ring.at[way, slot, d], ring.at[way, slot + 1, d], rs_s.at[way, slot, d], rs_r.at[way, slot + 1, d], device_id={'ep': side[way]}, device_id_type=MESH)

    def rs_wait(way, slot, d):
        @pl.when(d % PACK == 0)
        def _():
            rs_arrived(way, slot, d // PACK)

    def rs_send(way, slot, d):
        @pl.when(d % PACK == PACK - 1)
        def _():
            rs(way, slot, d // PACK).start()

    def rs_arrived(way, slot, d):
        pltpu.make_async_remote_copy(ring.at[way, slot, d], ring.at[way, slot, d], rs_s.at[way, slot, d], rs_r.at[way, slot, d], device_id={'ep': side[way]}, device_id_type=MESH).wait_recv()

    lane_rows = (pl.ds(0, half), pl.ds(half, half))

    def phase(dist, order, shards, last=False, events=False):
        width = shards // 2
        m_rows = shards * cap

        def shard_place(num):
            which = num % width
            step = dist if width == 1 else dist * (1 - 2 * which)
            return place(chip + step, jnp.where(num < width, core, other))

        def gather(num, carry):
            shard = shard_place(num)
            base = (me * n_exp * cap).astype(F32)
            row_num = lax.broadcasted_iota(jnp.int32, (slots, rows), 0)
            in_exp = row_num % spad
            want = jnp.where(in_exp < cap, (row_num // spad) * cap + in_exp, -7).astype(F32)
            codes = meta[shard, pl.ds(0, top_k), :] - base
            gates = meta[shard, pl.ds(top_k, top_k), :]
            hot = jnp.zeros((slots, rows), F32)
            gate = jnp.zeros((slots, rows), F32)
            for j in range(top_k):
                same = want == codes[j:j + 1, :]
                hot = jnp.where(same, 1.0, hot)
                gate = jnp.where(same, gates[j:j + 1, :], gate)
            slot_gate = jnp.broadcast_to(jnp.sum(gate, axis=1, keepdims=True), (slots, 128))
            first = pl.multiple_of(num * cap, 16)
            for e in range(n_exp):
                sgbuf[e, pl.ds(first, cap), :] = slot_gate[e * spad:e * spad + cap]
            ptbuf[num] = hot.T.astype(BF16)
            pick = hot.astype(BF16)
            for c in range(d_model // COLS):
                got = jnp.dot(pick, tok[shard, :, pl.ds(c * COLS, COLS)], preferred_element_type=F32).astype(BF16)
                for e in range(n_exp):
                    xbuf[e, pl.ds(first, cap), pl.ds(c * COLS, COLS)] = got[e * spad:e * spad + cap]
            return carry

        lax.fori_loop(0, shards, gather, 0)

        def up_step(step, carry):
            idx = step * 2
            slot = idx % n_w
            load_up(idx, slot, finish)
            e, col = step // n_f, pl.multiple_of((step % n_f) * COLS, COLS)
            x = xbuf[e, pl.ds(0, m_rows), :]
            a = jnp.dot(x, wbuf[slot], preferred_element_type=F32)
            u = jnp.dot(x, wbuf[slot + 1], preferred_element_type=F32)
            hbuf[e, pl.ds(0, m_rows), pl.ds(col, COLS)] = (jax.nn.silu(a) * u).astype(BF16)

            @pl.when(idx + n_w < up_loads)
            def _():
                load_up(idx + n_w, slot, begin)

            @pl.when(idx + n_w >= up_loads)
            def _():
                for k in range(2):
                    load_down(idx + n_w + k - up_loads, slot + k, begin)
            if events:
                every = max(n_exp * n_f // max(n_events - 2, 1), 1)
                early = every * 3 // 4 - 1 if every > 1 else 0

                @pl.when((step % every == early) & (step // every < n_events - 2))
                def _():
                    second_half_event(step // every)
            return carry

        lax.fori_loop(0, n_exp * n_f, up_step, 0)

        def sib_share(d, waiting=False):
            count = order * n_d + d
            return pltpu.make_async_remote_copy(sib_out.at[d % 2, pl.ds(0, width)], sib_in.at[count % SIB_SLOTS, pl.ds(0, width)], ss_s.at[d % 2], ss_r.at[count % SIB_SLOTS], device_id={'ep': sib}, device_id_type=MESH)

        def close(d):
            count = order * n_d + d
            slot = count % SIB_SLOTS
            sib_share(d).wait_recv()
            mine = lambda i, r: own[d % 2, i, lane_rows[r], :] + sib_in[slot, i, lane_rows[r], :]
            if last:
                for way in range(2):
                    rs_wait(way, a_slot + far, d)
                    rs_wait(way, b_slot + far - 1, d)
                for r in range(2):
                    total = mine(0, r) + ring[r, a_slot + far, d // PACK, d % PACK] + ring[1 - r, b_slot + far - 1, d // PACK, d % PACK]
                    out[lane_rows[r], pl.ds(pl.multiple_of(d * COLS, COLS), COLS)] = total.astype(BF16)
            elif width == 1:
                for way in range(2):
                    ring[way, a_slot, d // PACK, d % PACK] = mine(0, way)
                    rs_send(way, a_slot, d)
            else:
                b_now = b_slot + far - 1 - dist
                a_now = a_slot + far - dist

                @pl.when(dist == far - 1)
                def _():
                    for way in range(2):
                        ring[way, b_slot, d // PACK, d % PACK] = mine(way, 1 - way)

                @pl.when(dist != far - 1)
                def _():
                    for way in range(2):
                        rs_wait(way, b_now, d)
                        ring[way, b_now, d // PACK, d % PACK] += mine(way, 1 - way)
                for way in range(2):
                    rs_send(way, b_now, d)
                for way in range(2):
                    rs_wait(way, a_now, d)
                    ring[way, a_now, d // PACK, d % PACK] += mine(way, way)
                    rs_send(way, a_now, d)

            @pl.when(count < total_chunks - SIB_SLOTS)
            def _():
                pl.semaphore_signal(credit, inc=1, device_id={'ep': sib}, device_id_type=MESH)

        def down_step(d, carry):
            for pair in range(n_exp // 2):
                idx = d * (n_exp // 2) + pair
                slot = (up_loads + idx) % n_w
                load_down(idx, slot, finish)
                for k in range(2):
                    e = pair * 2 + k
                    o = jnp.dot(hbuf[e, pl.ds(0, m_rows), :], wbuf[slot, pl.ds(k * d_ff, d_ff), :], preferred_element_type=F32)
                    g = sgbuf[e, pl.ds(0, m_rows), :]
                    o = o * jnp.concatenate([g] * (COLS // 128), axis=1)
                    for p in range(3):
                        cut = o.astype(BF16)
                        o = o - cut.astype(F32)
                        for i in range(shards):
                            obuf[i, pl.ds(p * slots + e * spad, cap), :] = cut[i * cap:(i + 1) * cap]

                @pl.when(up_loads + idx + n_w < loads)
                def _():
                    load_down(idx + n_w, slot, begin)
                if not last:
                    @pl.when((up_loads + idx + n_w >= loads) & ((up_loads + idx + n_w - loads) % 2 == 1))
                    def _():
                        load_up(up_loads + idx + n_w - loads - 1, slot - 1, begin)

            @pl.when(d >= 2)
            def _():
                sib_share(d).wait_send()

            @pl.when(order * n_d + d >= SIB_SLOTS)
            def _():
                pl.semaphore_wait(credit, 1)
            for i in list(range(width, shards)) + list(range(width)):
                pt = ptbuf[i]
                share = jnp.dot(pt, obuf[i, pl.ds(0, slots), :], preferred_element_type=F32)
                for p in range(1, 3):
                    share += jnp.dot(pt, obuf[i, pl.ds(p * slots, slots), :], preferred_element_type=F32)
                if i >= width:
                    sib_out[d % 2, i - width] = share
                else:
                    own[d % 2, i] = share
                if i == shards - 1:
                    sib_share(d).start()

            @pl.when(d >= 1)
            def _():
                close(d - 1)
            if events:
                for k in range(2):
                    @pl.when(d == max((k + 1) * n_d // 2 - 2, k))
                    def _():
                        second_half_event(n_events - 2 + k)
            return carry

        lax.fori_loop(0, n_d, down_step, 0)
        close(jnp.int32(n_d - 1))
        for d in range(n_d - 2, n_d):
            sib_share(d).wait_send()

    for way in range(2):
        if far <= meta_hops[way]:
            sib_meta(way, far, other).wait_recv()
        for ck in range(AG_CHUNKS):
            if ck != swap_ck:
                sib_msg(way, 0, far, ck, other).wait_recv()

        @pl.when(core == 0)
        def _():
            stay_sib(way).wait_recv()

        @pl.when(core == 1)
        def _():
            sib_msg(way, 0, far, swap_ck, other).wait_recv()
            guest_sib(way).wait_recv()
    phase(far, 0, 2, events=True)

    def middle(order, carry):
        dist = far - order
        for way in range(2):
            sib_meta(way, dist, other).wait_recv()
            for kind in range(2):
                for ck in range(AG_CHUNKS):
                    if kind == 0 and ck == swap_ck:
                        @pl.when((core == 1) | (dist != far - 1))
                        def _():
                            sib_msg(way, kind, dist, ck, other).wait_recv()
                    else:
                        sib_msg(way, kind, dist, ck, other).wait_recv()
        phase(dist, order, 4)
        return carry

    lax.fori_loop(1, far, middle, 0)
    own_meta(other).wait_recv()
    own_tok(other).wait_recv()
    phase(0, far, 2, last=True)

    own_meta(core).wait_send()
    own_tok(core).wait_send()
    for way in range(2):
        for hop in range(1, far + 1):
            if hop <= meta_hops[way]:
                ag_meta(way, hop, False)[0].wait_send()
                sib_meta(way, hop, core).wait_send()
            for kind in range(2):
                if hop <= far - kind:
                    for ck in range(AG_CHUNKS):
                        if kind == 0 and hop == far and ck == swap_ck:
                            @pl.when(core == 0)
                            def _():
                                ag(way, kind, hop, ck, False)[0].wait_send()
                                sib_msg(way, kind, hop, ck, core).wait_send()
                                guest(way, False).wait_send()
                                guest_sib(way).wait_send()

                            @pl.when(core == 1)
                            def _():
                                stay(way, False).wait_send()
                                stay_sib(way).wait_send()
                        else:
                            ag(way, kind, hop, ck, False)[0].wait_send()
                            sib_msg(way, kind, hop, ck, core).wait_send()

        def drain(d, carry):
            for slot in list(range(a_slot, a_slot + far)) + list(range(b_slot, b_slot + far - 1)):
                rs(way, slot, d).wait_send()
            return carry
        lax.fori_loop(0, n_d // PACK, drain, 0)


def group_layer(n, tokens, ids, gates, slot_ids, w_gate, w_up, w_down, cap):
    rows, d_model = tokens.shape
    top_k = ids.shape[0]
    n_exp, _, d_ff = w_gate.shape
    far = n // 4
    spad = (cap + 63) // 64 * 64
    slots = n_exp * spad
    n_d = d_model // COLS
    loads = 2 * n_exp * d_ff // COLS + n_d * n_exp // 2
    n_w = 8 if loads % 8 == 0 else 4
    any_spec = pl.BlockSpec(memory_space=pl.ANY)
    dma = pltpu.SemaphoreType.DMA
    ag_shape = (2, 2, far, AG_CHUNKS)
    return pl.pallas_call(
        functools.partial(moe_kernel, (n, cap, spad, n_w)),
        out_shape=pltpu.VMEM((rows, d_model), BF16),
        in_specs=[any_spec] * 7,
        out_specs=pl.BlockSpec(memory_space=pltpu.VMEM),
        scratch_shapes=[
            pltpu.VMEM((n, rows, d_model), BF16),
            pltpu.VMEM((n, 2 * top_k, rows), F32),
            pltpu.VMEM((2, top_k, rows), jnp.int32),
            pltpu.VMEM((2, 2 * far + 1, n_d // PACK, PACK, rows // 2, COLS), F32),
            pltpu.VMEM((SIB_SLOTS, 2, rows, COLS), F32),
            pltpu.VMEM((2, 2, rows, COLS), F32),
            pltpu.VMEM((2, 2, rows, COLS), F32),
            pltpu.VMEM((n_w, d_model, COLS), BF16),
            pltpu.VMEM((n_exp, 4 * cap, d_model), BF16),
            pltpu.VMEM((n_exp, 4 * cap, d_ff), BF16),
            pltpu.VMEM((4, 3 * slots, COLS), BF16),
            pltpu.VMEM((4, rows, slots), BF16),
            pltpu.VMEM((n_exp, 4 * cap, 128), F32),
            dma((3 + 2 * AG_CHUNKS,)), dma((n_w, 2)),
            dma(ag_shape), dma(ag_shape), dma((2, far)), dma((2, far)),
            dma(ag_shape), dma(ag_shape), dma((2, far)), dma((2, far)),
            dma((2,)), dma((2,)), dma((2, 2)), dma((2, 2)),
            dma((2, 2 * far + 1, n_d // PACK)), dma((2, 2 * far + 1, n_d // PACK)),
            dma((2,)), dma((SIB_SLOTS,)),
            pltpu.SemaphoreType.REGULAR,
        ],
        compiler_params=pltpu.CompilerParams(collective_id=0, has_side_effects=True, vmem_limit_bytes=58 << 20),
    )(tokens, ids, gates, slot_ids, w_gate, w_up, w_down)


def solution(mesh):
    group_size = mesh.shape['ep']
    row_spec = P(('dp', 'ep'), None)
    expert_spec = P('ep', None, None)

    def per_device(tokens, expert_ids, gate_wts, slot_ids, w_gate, w_up, w_down):
        tok_dev, top_k = expert_ids.shape
        cap = CAP_NUM * tok_dev * top_k // (CAP_DEN * w_gate.shape[0] * group_size)
        return group_layer(group_size, tokens, expert_ids.T, gate_wts.T, slot_ids.T, w_gate, w_up, w_down, cap)

    return jax.shard_map(per_device, mesh=mesh, in_specs=(row_spec, row_spec, row_spec, row_spec, expert_spec, expert_spec, expert_spec), out_specs=row_spec, check_vma=False)
```
